32 devices in a mesh: cell: 8 (over z, x), grp: 4 (over y, core).
Axes of the slice: x: 2, y: 2, z: 4, core: 2. Of those that a mesh axis runs over, the one named last changes fastest.
Arguments:
- atom_sites: float32 [3, 16384], P(None, ('cell', 'grp')), may hold values from 0 to 8, as said below
- grid_points: float32 [3, 12288], P(None, ('cell', 'grp')), may hold values from 0 to 8, as said below
- dipole_guess: float32 [3, 16384], P(None, ('cell', 'grp')), may hold values from -2 to 2
- fixed_field: float32 [3, 16384], P(None, ('cell', 'grp')), may hold values from -1800 to 1800
- polarisability: float32 [16384], P(('cell', 'grp')), may hold values from 0.0005 to 0.002
- base_charge: float32 [12288], P(('cell', 'grp')), may hold values from -12 to 12
- response: float32 [12288], P(('cell', 'grp')), may hold values from 0.02 to 0.2
- near_blocks: int32 [128, 8], P(('cell', 'grp')), may hold values from 0 to 47, as said below
- grid_blocks: int32 [128, 4], P(('cell', 'grp')), may hold values from 0 to 35, as said below
- source_blocks: int32 [96, 8], P(('cell', 'grp')), may hold values from 0 to 47, as said below
Outputs:
- dipoles: float32 [3, 16384], P(None, ('cell', 'grp'))
- qm_charges: float32 [12288], P(('cell', 'grp'))
The draws below stay inside these ranges and needn't reach their ends.
Inputs may be any that keep to these rules, and one draw needn't show every extreme that they name: `atom_sites`: atom a has first coordinate in [c, c + 1) with c = a // 2048, the other two in [0, 1). `grid_points`: grid point g has first coordinate in [c, c + 1) with c = g // 1536, the other two in [0, 1). `near_blocks`: each row holds 8 distinct MM window indices, never the block's own index 16 + b % 16. `grid_blocks`: each row holds 4 distinct grid window indices. `source_blocks`: each row holds 8 distinct MM window indices.
All inputs are finite; a program needn't handle non-finite values.
Results may differ from the reference program's by a relative error of at most 0.0003.
Values sent between devices are 32-bit elements; how exact they have to be, the bound alone decides.
A program may use at most 64 MiB of HBM per device.

```python
import math
import jax
import jax.numpy as jnp
from jax import lax

BLOCK = 128
NB = 8
NQ = 4
NM = 8
ITERS = 3
CELLS = 8
CELL_BLK = 16
CELL_GBLK = 12
CELL_ATOMS = 2048
CELL_GRID = 1536
BLOCKS = 128
GBLOCKS = 96
ATOMS = 16384
GRID = 12288


def place_points(key, per_cell):
    uniform_unit = jax.random.uniform(key, (3, CELLS * per_cell), jnp.float32)
    shift_x = (jnp.arange(CELLS * per_cell, dtype=jnp.int32) // per_cell).astype(jnp.float32)
    return jnp.stack([uniform_unit[0] + shift_x, uniform_unit[1], uniform_unit[2]])


def window_lists(key, row_count, span, picks, cell_rows, exclude_own):
    scores = jax.random.randint(key, (row_count, span), 0, 1 << 20, dtype=jnp.int32) * span
    scores = scores + jnp.arange(span, dtype=jnp.int32)[None, :]
    if exclude_own:
        own_rows = cell_rows + jnp.arange(row_count, dtype=jnp.int32) % cell_rows
        scores = jnp.where(jnp.arange(span, dtype=jnp.int32)[None, :] == own_rows[:, None], -1, scores)
    return lax.top_k(scores, picks)[1].astype(jnp.int32)


def draw_atom_sites(key, part):
    return place_points(jax.random.fold_in(key, 11), CELL_ATOMS)


def draw_grid_points(key, part):
    return place_points(jax.random.fold_in(key, 12), CELL_GRID)


def draw_near_blocks(key, part):
    return window_lists(jax.random.fold_in(key, 21), BLOCKS, 3 * CELL_BLK, NB, CELL_BLK, True)


def draw_grid_blocks(key, part):
    return window_lists(jax.random.fold_in(key, 22), BLOCKS, 3 * CELL_GBLK, NQ, CELL_GBLK, False)


def draw_source_blocks(key, part):
    return window_lists(jax.random.fold_in(key, 23), GBLOCKS, 3 * CELL_BLK, NM, CELL_BLK, False)


def level_of(own_key, dims, shards, low, top_value):
    def one(dim, blocks):
        steps = jax.random.uniform(jax.random.fold_in(jax.random.fold_in(own_key, 6), dim), (blocks,), jnp.float32, low / len(shards), top_value / len(shards))
        return jnp.repeat(jnp.exp(steps), dims[dim] // blocks).reshape((-1,) + (1,) * (len(dims) - dim - 1))

    gain = one(*shards[0])
    for cut in shards[1:]:
        gain = gain * one(*cut)
    return gain


def scatter_about(own_key, extent, deviation, bound, shards=(), kind=jnp.bfloat16):
    gain = level_of(own_key, extent, shards, -0.22, 0.18) if shards else 1.0
    values = jax.random.normal(own_key, extent, jnp.float32) * deviation * gain
    return jnp.minimum(jnp.maximum(values, -bound), bound).astype(kind)


def setup_inputs(seed: int = 0) -> dict:
    arg_keys = jax.random.split(jax.random.key(seed), 11)
    atom_sites = draw_atom_sites(jax.random.fold_in(arg_keys[10], 71), 0)
    grid_points = draw_grid_points(jax.random.fold_in(arg_keys[10], 71), 0)
    dipole_guess = scatter_about(arg_keys[2], (3, ATOMS), 0.3, 2.0, ((1, 32),), jnp.float32)
    fixed_field = scatter_about(arg_keys[3], (3, ATOMS), 300.0, 1800.0, ((1, 32),), jnp.float32)
    polarisability = jnp.clip(jnp.exp(math.log(0.002) - 1.3862944 * jax.random.uniform(arg_keys[4], (ATOMS,), jnp.float32) ** level_of(arg_keys[4], (ATOMS,), ((0, 32),), -0.2, 0.2)), 0.0005, 0.002)
    base_charge = scatter_about(arg_keys[5], (GRID,), 2.0, 12.0, ((0, 32),), jnp.float32)
    response = jnp.clip(jnp.exp(math.log(0.2) - 2.3025851 * jax.random.uniform(arg_keys[6], (GRID,), jnp.float32) ** level_of(arg_keys[6], (GRID,), ((0, 32),), -0.2, 0.2)), 0.02, 0.2)
    near_blocks = draw_near_blocks(jax.random.fold_in(arg_keys[10], 71), 0)
    grid_blocks = draw_grid_blocks(jax.random.fold_in(arg_keys[10], 71), 0)
    source_blocks = draw_source_blocks(jax.random.fold_in(arg_keys[10], 71), 0)
    return dict(atom_sites=atom_sites, grid_points=grid_points, dipole_guess=dipole_guess, fixed_field=fixed_field, polarisability=polarisability, base_charge=base_charge, response=response, near_blocks=near_blocks, grid_blocks=grid_blocks, source_blocks=source_blocks)


soften_sq = 0.04

def pick_tile(tile_set, slot_index):
    return lax.dynamic_index_in_dim(tile_set, slot_index, 1, keepdims=False)

def pair_geometry(targets, sources):
    delta_x = targets[0][:, None] - sources[0][None, :]
    delta_y = targets[1][:, None] - sources[1][None, :]
    delta_z = targets[2][:, None] - sources[2][None, :]
    inverse = 1.0 / jnp.sqrt(delta_x * delta_x + delta_y * delta_y + delta_z * delta_z + soften_sq)
    inv_cube = inverse * inverse * inverse
    return (delta_x, delta_y, delta_z, inv_cube, inv_cube * inverse * inverse)

def dipole_field(targets, sources, moments, keep_mask):
    delta_x, delta_y, delta_z, inv_cube, inv_fifth = pair_geometry(targets, sources)
    projected = moments[0][None, :] * delta_x + moments[1][None, :] * delta_y + moments[2][None, :] * delta_z
    radial = 3.0 * projected * inv_fifth * keep_mask
    direct = inv_cube * keep_mask
    return jnp.stack([lax.optimization_barrier(jnp.sum(radial * delta_x - moments[0][None, :] * direct, axis=1)), lax.optimization_barrier(jnp.sum(radial * delta_y - moments[1][None, :] * direct, axis=1)), lax.optimization_barrier(jnp.sum(radial * delta_z - moments[2][None, :] * direct, axis=1))])

def charge_field(targets, sources, charges):
    delta_x, delta_y, delta_z, inv_cube, inv_fifth = pair_geometry(targets, sources)
    weight = charges[None, :] * inv_cube
    return jnp.stack([lax.optimization_barrier(jnp.sum(weight * delta_x, axis=1)), lax.optimization_barrier(jnp.sum(weight * delta_y, axis=1)), lax.optimization_barrier(jnp.sum(weight * delta_z, axis=1))])

def dipole_potential(targets, sources, moments):
    delta_x, delta_y, delta_z, inv_cube, inv_fifth = pair_geometry(targets, sources)
    projected = moments[0][None, :] * delta_x + moments[1][None, :] * delta_y + moments[2][None, :] * delta_z
    return lax.optimization_barrier(jnp.sum(projected * inv_cube, axis=1))

def far_geometry(targets, cell_here, cell_count):
    centres = jnp.arange(cell_count, dtype=jnp.int32).astype(jnp.float32) + 0.5
    delta_x = targets[0][None, :] - centres[:, None]
    delta_y = targets[1][None, :] - 0.5
    delta_z = targets[2][None, :] - 0.5
    far_mask = (jnp.abs(jnp.arange(cell_count, dtype=jnp.int32) - cell_here) >= 2).astype(jnp.float32)[:, None]
    inverse = 1.0 / jnp.sqrt(delta_x * delta_x + delta_y * delta_y + delta_z * delta_z + soften_sq)
    inv_cube = inverse * inverse * inverse * far_mask
    return (delta_x, delta_y, delta_z, inv_cube, inv_cube * inverse * inverse)

def far_field(targets, cell_here, moments, charges):
    delta_x, delta_y, delta_z, inv_cube, inv_fifth = far_geometry(targets, cell_here, charges.shape[0])
    projected = moments[:, 0:1] * delta_x + moments[:, 1:2] * delta_y + moments[:, 2:3] * delta_z
    radial = 3.0 * projected * inv_fifth
    coulomb = charges[:, None] * inv_cube
    return jnp.stack([lax.optimization_barrier(jnp.sum(radial * delta_x - moments[:, 0:1] * inv_cube + coulomb * delta_x, axis=0)), lax.optimization_barrier(jnp.sum(radial * delta_y - moments[:, 1:2] * inv_cube + coulomb * delta_y, axis=0)), lax.optimization_barrier(jnp.sum(radial * delta_z - moments[:, 2:3] * inv_cube + coulomb * delta_z, axis=0))])

def far_potential(targets, cell_here, moments):
    delta_x, delta_y, delta_z, inv_cube, inv_fifth = far_geometry(targets, cell_here, moments.shape[0])
    projected = moments[:, 0:1] * delta_x + moments[:, 1:2] * delta_y + moments[:, 2:3] * delta_z
    return lax.optimization_barrier(jnp.sum(projected * inv_cube, axis=0))

def atom_block(targets, own_slot, near_list, grid_list, site_tiles, dipole_tiles, point_tiles, charge_tiles, cell_here, moments, charge_sums):
    tile_width = targets.shape[1]
    self_mask = 1.0 - jnp.eye(tile_width, dtype=jnp.float32)
    accumulated = dipole_field(targets, pick_tile(site_tiles, own_slot), pick_tile(dipole_tiles, own_slot), self_mask)

    def near_step(member, carried):
        other_slot = near_list[member]
        return carried + dipole_field(targets, pick_tile(site_tiles, other_slot), pick_tile(dipole_tiles, other_slot), 1.0)
    accumulated = lax.fori_loop(0, near_list.shape[0], near_step, accumulated)

    def grid_step(member, carried):
        other_slot = grid_list[member]
        return carried + charge_field(targets, pick_tile(point_tiles, other_slot), lax.dynamic_index_in_dim(charge_tiles, other_slot, 0, keepdims=False))
    accumulated = lax.fori_loop(0, grid_list.shape[0], grid_step, accumulated)
    return accumulated + far_field(targets, cell_here, moments, charge_sums)

def grid_block(targets, source_list, site_tiles, dipole_tiles, cell_here, dipole_sums):

    def near_step(member, carried):
        other_slot = source_list[member]
        return carried + dipole_potential(targets, pick_tile(site_tiles, other_slot), pick_tile(dipole_tiles, other_slot))
    accumulated = lax.fori_loop(0, source_list.shape[0], near_step, jnp.zeros((targets.shape[1],), jnp.float32))
    return accumulated + far_potential(targets, cell_here, dipole_sums)

def cell_table(dipoles, charges, grid_points):
    dipole_sums = lax.optimization_barrier(jnp.sum(dipoles.reshape(3, CELLS, CELL_ATOMS), axis=2)).T
    charge_cells = charges.reshape(CELLS, CELL_GRID)
    centres = jnp.stack([jnp.arange(CELLS, dtype=jnp.int32).astype(jnp.float32) + 0.5, jnp.full((CELLS,), 0.5, jnp.float32), jnp.full((CELLS,), 0.5, jnp.float32)])
    offsets = grid_points.reshape(3, CELLS, CELL_GRID) - centres[:, :, None]
    charge_sums = lax.optimization_barrier(jnp.sum(charge_cells, axis=1))
    grid_moments = lax.optimization_barrier(jnp.sum(charge_cells[None, :, :] * offsets, axis=2)).T
    return (dipole_sums, charge_sums, grid_moments)

def reference(atom_sites, grid_points, dipole_guess, fixed_field, polarisability, base_charge, response, near_blocks, grid_blocks, source_blocks):
    target_tiles = atom_sites.reshape(3, BLOCKS, BLOCK)
    grid_targets = grid_points.reshape(3, GBLOCKS, BLOCK)
    site_tiles = jnp.pad(target_tiles, ((0, 0), (CELL_BLK, CELL_BLK), (0, 0)))
    point_tiles = jnp.pad(grid_targets, ((0, 0), (CELL_GBLK, CELL_GBLK), (0, 0)))
    dipoles = dipole_guess
    charges = base_charge
    for iteration in range(ITERS):
        dipole_sums, charge_sums, grid_moments = cell_table(dipoles, charges, grid_points)
        moments = dipole_sums + grid_moments
        dipole_tiles = jnp.pad(dipoles.reshape(3, BLOCKS, BLOCK), ((0, 0), (CELL_BLK, CELL_BLK), (0, 0)))
        charge_tiles = jnp.pad(charges.reshape(GBLOCKS, BLOCK), ((CELL_GBLK, CELL_GBLK), (0, 0)))

        def one_atom_block(block_index):
            cell_here = block_index // CELL_BLK
            window_start = cell_here * CELL_BLK
            grid_start = cell_here * CELL_GBLK
            return atom_block(pick_tile(target_tiles, block_index), block_index - window_start + CELL_BLK, near_blocks[block_index], grid_blocks[block_index], lax.dynamic_slice_in_dim(site_tiles, window_start, 3 * CELL_BLK, 1), lax.dynamic_slice_in_dim(dipole_tiles, window_start, 3 * CELL_BLK, 1), lax.dynamic_slice_in_dim(point_tiles, grid_start, 3 * CELL_GBLK, 1), lax.dynamic_slice_in_dim(charge_tiles, grid_start, 3 * CELL_GBLK, 0), cell_here, moments, charge_sums)

        def one_grid_block(block_index):
            cell_here = block_index // CELL_GBLK
            window_start = cell_here * CELL_BLK
            return grid_block(pick_tile(grid_targets, block_index), source_blocks[block_index], lax.dynamic_slice_in_dim(site_tiles, window_start, 3 * CELL_BLK, 1), lax.dynamic_slice_in_dim(dipole_tiles, window_start, 3 * CELL_BLK, 1), cell_here, dipole_sums)
        induced_field = lax.map(one_atom_block, jnp.arange(BLOCKS, dtype=jnp.int32))
        induced_field = jnp.transpose(induced_field, (1, 0, 2)).reshape(3, ATOMS)
        potential = lax.map(one_grid_block, jnp.arange(GBLOCKS, dtype=jnp.int32)).reshape(GRID)
        dipoles = polarisability[None, :] * (fixed_field + induced_field)
        charges = base_charge - response * potential
    return (dipoles, charges)
```

```python
import functools
import math

import jax
import jax.numpy as jnp
from jax import lax
from jax.experimental import pallas as pl
from jax.experimental.pallas import tpu as pltpu
from jax.sharding import PartitionSpec as P

BLOCK = 128
SUB = 8
GROUPS = BLOCK // SUB
UNROLL = 8
HALVES = GROUPS // UNROLL
ITERS = 3
MESH = pl.DeviceIdType.MESH

soften_sq = 0.04


def body(dims, *refs):
    cells, grps, na, ng, nb, nq, nm = dims
    args, (out_dip, out_q), held = refs[:10], refs[10:12], refs[12:22]
    near_s, grid_s, source_s, sites, points, guess, fixed, pol, base, resp = held
    sit, pts = refs[22:24]
    mus = refs[24 : 24 + ITERS]
    chg = (None,) + refs[24 + ITERS : 23 + 2 * ITERS]
    tab = refs[23 + 2 * ITERS : 23 + 3 * ITERS]
    rest = refs[23 + 3 * ITERS :]
    tgt_a, tgt_g, geo, sgeo, cgeo, pgeo, fgeo_a, fgeo_g, acc_a, acc_g = rest[:10]
    load_sem, send_sem, recv_sem, far_send, far_recv = rest[10:]
    cell = lax.axis_index("cell")
    grp = lax.axis_index("grp")
    has_prev = cell > 0
    has_next = cell < cells - 1
    own = grps + grp
    cell_f = cell.astype(jnp.float32)
    centre = (cell_f + 0.5, 0.5, 0.5)
    pieces = 3 * grps
    order = sorted(range(grps), key=lambda d: (abs(2 * d - grps), d))

    site_msg = (sit, 3 * na, 0)
    point_msg = (pts, 4 * ng, 1)
    mu_msg = [(mus[it], 3 * na, 2 + it) for it in range(ITERS)]
    charge_msg = [None] + [(chg[it], ng, 1 + ITERS + it) for it in range(1, ITERS)]

    def vec_row(ref, a, b):
        return ref[a : a + 1, b * BLOCK : (b + 1) * BLOCK]

    def flat_row(ref, b):
        return ref[b * BLOCK : (b + 1) * BLOCK].reshape(1, BLOCK)

    lanes = lax.broadcasted_iota(jnp.int32, (SUB, BLOCK), 1)
    subs = lax.broadcasted_iota(jnp.int32, (SUB, BLOCK), 0)
    diag = lanes - subs

    barrier = pltpu.get_barrier_semaphore()

    def greet(c, g):
        pl.semaphore_signal(barrier, inc=1, device_id=(c, g), device_id_type=MESH)

    def each_other_cell(act):
        def step(n, carry):
            c = lax.rem(cell + n, cells)
            for d in range(grps):
                act(c, lax.rem(grp + d, grps))
            return carry

        lax.fori_loop(1, cells, step, 0)

    loads = [
        pltpu.make_async_copy(src, dst, load_sem.at[n])
        for n, (src, dst) in enumerate(zip(args, held))
    ]
    for n in (3, 5, 4, 8, 0, 1, 2, 6, 7, 9):
        loads[n].start()
    each_other_cell(greet)
    for d in range(1, grps):
        greet(cell, lax.rem(grp + d, grps))

    def clear(slot):
        for buf, rows, _ in [site_msg, point_msg] + mu_msg + charge_msg[1:]:
            buf[slot * grps * rows : (slot + 1) * grps * rows] = jnp.zeros((grps * rows, 1, BLOCK), jnp.float32)

    for it in range(ITERS):
        for g in range(grps):
            tab[it][g * cells + cell] = jnp.zeros((1, BLOCK), jnp.float32)
    pl.when(jnp.logical_not(has_prev))(lambda: clear(0))
    pl.when(jnp.logical_not(has_next))(lambda: clear(2))

    for n in (3, 5, 4, 8):
        loads[n].wait()

    for b in range(na):
        for a in range(3):
            sit[own * 3 * na + b * 3 + a] = vec_row(sites, a, b)
            mus[0][own * 3 * na + b * 3 + a] = vec_row(guess, a, b)
    for b in range(ng):
        for a in range(3):
            pts[own * 4 * ng + b * 4 + a] = vec_row(points, a, b)
        pts[own * 4 * ng + b * 4 + 3] = flat_row(base, b)

    def inverse_of(dx, dy, dz):
        return lax.rsqrt(dx * dx + dy * dy + dz * dz + soften_sq)

    def store_dipole_pair(ref, slot, targets, source, self_mask):
        dx, dy, dz = (t - s for t, s in zip(targets, source))
        inv = inverse_of(dx, dy, dz)
        cube = inv * inv * inv
        weight = cube * lax.rsqrt(inv) * math.sqrt(3.0)
        ref[slot] = dx * weight
        ref[slot + 1] = dy * weight
        ref[slot + 2] = dz * weight
        ref[slot + 3] = cube if self_mask is None else jnp.where(self_mask, 0.0, cube)

    def store_charge_pair(ref, slot, targets, source):
        dx, dy, dz = (t - s for t, s in zip(targets, source))
        inv = inverse_of(dx, dy, dz)
        cube = inv * inv * inv
        ref[slot] = dx * cube
        ref[slot + 1] = dy * cube
        ref[slot + 2] = dz * cube

    def column_sum(x):
        return jnp.sum(x, axis=0, keepdims=True)

    def wide(row):
        return jnp.broadcast_to(row, (SUB, BLOCK))

    def targets_of(ref, b, group):
        return [ref[b, a, pl.ds(group * SUB, SUB), :] for a in range(3)]

    def piece_copy(msg, slot, c, g):
        buf, rows, kind = msg
        return pltpu.make_async_remote_copy(
            src_ref=buf.at[pl.ds(own * rows, rows)],
            dst_ref=buf.at[pl.ds((slot * grps + grp) * rows, rows)],
            send_sem=send_sem.at[kind, slot * grps + g],
            recv_sem=recv_sem.at[kind, slot * grps + grp],
            device_id=(c, g),
            device_id_type=MESH,
        )

    def for_all(msg, act):
        @pl.when(has_prev)
        def _():
            for d in order:
                g = lax.rem(grp + d, grps)
                act(piece_copy(msg, 2, cell - 1, g))

        @pl.when(has_next)
        def _():
            for d in order:
                g = lax.rem(grp + d, grps)
                act(piece_copy(msg, 0, cell + 1, g))

        for d in order:
            if d:
                g = lax.rem(grp + d, grps)
                act(piece_copy(msg, 1, cell, g))

    def arrival(msg, p, c, g):
        buf, rows, kind = msg
        pltpu.make_async_remote_copy(
            src_ref=buf.at[pl.ds(p * rows, rows)],
            dst_ref=buf.at[pl.ds(p * rows, rows)],
            send_sem=send_sem.at[kind, p],
            recv_sem=recv_sem.at[kind, p],
            device_id=(c, g),
            device_id_type=MESH,
        ).wait_recv()

    def all_arrive(msg):
        for d in range(1, grps):
            g = lax.rem(grp + d, grps)
            arrival(msg, grps + g, cell, g)

        @pl.when(has_prev)
        def _():
            for g in range(grps):
                arrival(msg, g, cell - 1, g)

        @pl.when(has_next)
        def _():
            for g in range(grps):
                arrival(msg, 2 * grps + g, cell + 1, g)

    def start(copy):
        copy.start()

    def finish(copy):
        copy.wait_send()

    def far_row(it, c, g):
        return tab[it].at[pl.ds(g * cells + c, 1)]

    def far_copy(it, c, g):
        return pltpu.make_async_remote_copy(
            src_ref=far_row(it, cell, grp),
            dst_ref=far_row(it, cell, grp),
            send_sem=far_send.at[it],
            recv_sem=far_recv.at[it],
            device_id=(c, g),
            device_id_type=MESH,
        )

    def far_all(it):
        rows = tab[it].at[pl.ds(0, (cells - 1) * grps)]
        return pltpu.make_async_remote_copy(
            src_ref=rows,
            dst_ref=rows,
            send_sem=far_send.at[it],
            recv_sem=far_recv.at[it],
            device_id=(lax.rem(cell + 1, cells), grp),
            device_id_type=MESH,
        )

    def charge_row(it, w):
        return pts[w * 4 + 3] if it == 0 else chg[it][w]

    def own_sums(it):
        rows = []
        for a in range(3):
            total = mus[it][own * 3 * na + a]
            for b in range(1, na):
                total = total + mus[it][own * 3 * na + b * 3 + a]
            rows.append(total)
        q = [charge_row(it, own * ng + b) for b in range(ng)]
        rows.append(functools.reduce(jnp.add, q))
        for a in range(3):
            rows.append(functools.reduce(jnp.add, [q[b] * (vec_row(points, a, b) - centre[a]) for b in range(ng)]))
        tile = jnp.zeros((SUB, BLOCK), jnp.float32)
        for n, row in enumerate(rows):
            tile = jnp.where(subs == n, wide(row), tile)
        sums = jnp.sum(tile, axis=1, keepdims=True)
        tab[it][grp * cells + cell] = column_sum(jnp.where(diag == 0, sums, 0.0))

    def far_sums(it):
        total = tab[it][0:cells, 0, :]
        for g in range(1, grps):
            total = total + tab[it][g * cells : (g + 1) * cells, 0, :]
        return [jnp.broadcast_to(total[:, n : n + 1], (cells, BLOCK)) for n in range(7)]

    def site_rows(w):
        return [wide(sit[w * 3 + a]) for a in range(3)]

    def point_rows(w):
        return [wide(pts[w * 4 + a]) for a in range(3)]

    def mu_rows(it, w):
        return [wide(mus[it][w * 3 + a]) for a in range(3)]

    def near_geometry(i, carry):
        b = lax.div(i, HALVES)
        first = lax.rem(i, HALVES) * UNROLL
        for k in range(nb):
            source = site_rows(near_s[b, k])
            for t in range(UNROLL):
                slot = ((i * UNROLL + t) * nb + k) * 4
                store_dipole_pair(geo, slot, targets_of(tgt_a, b, first + t), source, None)
        return carry

    def charge_geometry(i, carry):
        b = lax.div(i, HALVES)
        first = lax.rem(i, HALVES) * UNROLL
        for k in range(nq):
            source = point_rows(grid_s[b, k])
            for t in range(UNROLL):
                slot = ((i * UNROLL + t) * nq + k) * 3
                store_charge_pair(cgeo, slot, targets_of(tgt_a, b, first + t), source)
        return carry

    def grid_geometry(i, carry):
        b = lax.div(i, HALVES)
        first = lax.rem(i, HALVES) * UNROLL
        for k in range(nm):
            source = site_rows(source_s[b, k])
            for t in range(UNROLL):
                slot = ((i * UNROLL + t) * nm + k) * 3
                store_charge_pair(pgeo, slot, targets_of(tgt_g, b, first + t), source)
        return carry

    def self_atoms(it, i, carry):
        b = lax.div(i, HALVES)
        mu = mu_rows(it, own * na + b)
        for t in range(UNROLL):
            slot = (i * UNROLL + t) * 4
            u = [sgeo[slot + a] for a in range(3)]
            cube = sgeo[slot + 3]
            proj = u[0] * mu[0] + u[1] * mu[1] + u[2] * mu[2]
            for a in range(3):
                acc_a[(i * UNROLL + t) * 3 + a] = u[a] * proj - cube * mu[a]
        return carry

    def near_atoms(it, i, carry):
        b = lax.div(i, HALVES)
        acc = [[acc_a[(i * UNROLL + t) * 3 + a] for a in range(3)] for t in range(UNROLL)]
        for k in range(nb):
            mu = mu_rows(it, near_s[b, k])
            for t in range(UNROLL):
                slot = ((i * UNROLL + t) * nb + k) * 4
                u = [geo[slot + a] for a in range(3)]
                cube = geo[slot + 3]
                proj = u[0] * mu[0] + u[1] * mu[1] + u[2] * mu[2]
                for a in range(3):
                    acc[t][a] = acc[t][a] + (u[a] * proj - cube * mu[a])
        for t in range(UNROLL):
            for a in range(3):
                acc_a[(i * UNROLL + t) * 3 + a] = acc[t][a]
        return carry

    def near_grid(it, i, carry):
        b = lax.div(i, HALVES)
        acc = [None] * UNROLL
        for k in range(nm):
            mu = mu_rows(it, source_s[b, k])
            for t in range(UNROLL):
                slot = ((i * UNROLL + t) * nm + k) * 3
                term = pgeo[slot] * mu[0] + pgeo[slot + 1] * mu[1] + pgeo[slot + 2] * mu[2]
                acc[t] = term if k == 0 else acc[t] + term
        for t in range(UNROLL):
            acc_g[i * UNROLL + t] = acc[t]
        return carry

    def gather_lanes(tiles):
        row = jnp.zeros((SUB, BLOCK), jnp.float32)
        for t, tile in enumerate(tiles):
            total = jnp.sum(tile, axis=1, keepdims=True)
            row = jnp.where(diag == t * SUB, total, row)
        return column_sum(row)

    def atom_fields(it):
        rows = []
        for b in range(na):
            q = [wide(charge_row(it, grid_s[b, k])) for k in range(nq)]
            tiles = [[], [], []]
            for t in range(GROUPS):
                n = b * GROUPS + t
                for a in range(3):
                    terms = [cgeo[(n * nq + k) * 3 + a] * q[k] for k in range(nq)]
                    tiles[a].append(acc_a[n * 3 + a] + functools.reduce(jnp.add, terms))
            rows.append([gather_lanes(tiles[a]) for a in range(3)])
        return rows

    def grid_fields():
        return [gather_lanes([acc_g[b * GROUPS + t] for t in range(GROUPS)]) for b in range(ng)]

    def store_far(ref, n, row_of):
        c = lax.broadcasted_iota(jnp.int32, (cells, BLOCK), 0)
        dx = row_of(0) - (c.astype(jnp.float32) + 0.5)
        dy = jnp.broadcast_to(row_of(1) - 0.5, (cells, BLOCK))
        dz = jnp.broadcast_to(row_of(2) - 0.5, (cells, BLOCK))
        inv = inverse_of(dx, dy, dz)
        cube = jnp.where(jnp.abs(c - cell) >= 2, inv * inv * inv, 0.0)
        for m, x in enumerate((dx, dy, dz, cube, cube * inv * inv * 3.0)):
            ref[n * 5 + m] = x

    def finish_atoms(it, near, sums):
        moments = [sums[a] + sums[4 + a] for a in range(3)]
        for b in range(na):
            delta = [fgeo_a[b * 5 + a] for a in range(3)]
            cube, fifth = fgeo_a[b * 5 + 3], fgeo_a[b * 5 + 4]
            radial = fifth * (moments[0] * delta[0] + moments[1] * delta[1] + moments[2] * delta[2])
            radial = radial + sums[3] * cube
            for a in range(3):
                far = column_sum(radial * delta[a] - moments[a] * cube)
                new = flat_row(pol, b) * (vec_row(fixed, a, b) + (near[b][a] + far))
                if it + 1 < ITERS:
                    mus[it + 1][own * 3 * na + b * 3 + a] = new
                else:
                    out_dip[a : a + 1, b * BLOCK : (b + 1) * BLOCK] = new

    def finish_grid(it, near, sums):
        for b in range(ng):
            delta = [fgeo_g[b * 5 + a] for a in range(3)]
            proj = sums[0] * delta[0] + sums[1] * delta[1] + sums[2] * delta[2]
            far = column_sum(proj * fgeo_g[b * 5 + 3])
            new = flat_row(base, b) - flat_row(resp, b) * (near[b] + far)
            if it + 1 < ITERS:
                chg[it + 1][own * ng + b] = new
            else:
                out_q[b * BLOCK : (b + 1) * BLOCK] = new.reshape(BLOCK)

    atom_steps, grid_steps = na * HALVES, ng * HALVES

    pl.semaphore_wait(barrier, cells * grps - 1)
    for_all(site_msg, start)
    for_all(mu_msg[0], start)
    for_all(point_msg, start)
    own_sums(0)
    each_other_cell(lambda c, g: far_copy(0, c, g).start())

    for a in range(3):
        for b in range(na):
            tgt_a[b, a] = jnp.transpose(jnp.broadcast_to(vec_row(sites, a, b), (BLOCK, BLOCK)))
        for b in range(ng):
            tgt_g[b, a] = jnp.transpose(jnp.broadcast_to(vec_row(points, a, b), (BLOCK, BLOCK)))
    for b in range(na):
        source = [wide(vec_row(sites, a, b)) for a in range(3)]
        for t in range(GROUPS):
            store_dipole_pair(sgeo, (b * GROUPS + t) * 4, targets_of(tgt_a, b, t), source, diag == t * SUB)
    lax.fori_loop(0, atom_steps, functools.partial(self_atoms, 0), 0)
    for b in range(na):
        store_far(fgeo_a, b, lambda a: vec_row(sites, a, b))
    for b in range(ng):
        store_far(fgeo_g, b, lambda a: vec_row(points, a, b))
    for n in (0, 1, 2, 6, 7, 9):
        loads[n].wait()

    all_arrive(site_msg)
    lax.fori_loop(0, atom_steps, near_geometry, 0)

    for it in range(ITERS):
        last = it + 1 == ITERS
        all_arrive(mu_msg[it])
        lax.fori_loop(0, atom_steps, functools.partial(near_atoms, it), 0)
        if last:
            lax.fori_loop(0, grid_steps, functools.partial(near_grid, it), 0)
        if it == 0:
            all_arrive(point_msg)
            lax.fori_loop(0, atom_steps, charge_geometry, 0)
        else:
            all_arrive(charge_msg[it])
        far_all(it).wait_recv()
        sums = far_sums(it)
        finish_atoms(it, atom_fields(it), sums)
        if last:
            finish_grid(it, grid_fields(), sums)
            break
        for_all(mu_msg[it + 1], start)
        if it == 0:
            lax.fori_loop(0, grid_steps, grid_geometry, 0)
        lax.fori_loop(0, grid_steps, functools.partial(near_grid, it), 0)
        finish_grid(it, grid_fields(), sums)
        for_all(charge_msg[it + 1], start)
        own_sums(it + 1)
        each_other_cell(lambda c, g: far_copy(it + 1, c, g).start())
        lax.fori_loop(0, atom_steps, functools.partial(self_atoms, it + 1), 0)

    for msg in [site_msg, point_msg] + mu_msg + charge_msg[1:]:
        for_all(msg, finish)
    for it in range(ITERS):
        far_all(it).wait_send()


def hand_over(dip, q, out_dip, out_q, sem):
    copies = [
        pltpu.make_async_copy(dip, out_dip, sem.at[0]),
        pltpu.make_async_copy(q, out_q, sem.at[1]),
    ]
    for copy in copies:
        copy.start()
    for copy in copies:
        copy.wait()


def solution(mesh):
    cells, grps = mesh.shape["cell"], mesh.shape["grp"]

    def step(sites, points, guess, fixed, pol, base, resp, near, grid, source):
        na, nb = near.shape
        nq = grid.shape[1]
        ng, nm = source.shape
        f32 = jnp.float32
        args = (near, grid, source, sites, points, guess, fixed, pol, base, resp)
        args = tuple(pltpu.with_memory_space_constraint(x, pltpu.HBM) for x in args)
        vmem = pl.BlockSpec(memory_space=pltpu.VMEM)
        hbm = pl.BlockSpec(memory_space=pltpu.HBM)
        dma = pltpu.SemaphoreType.DMA
        outs = (jax.ShapeDtypeStruct(sites.shape, f32), jax.ShapeDtypeStruct(base.shape, f32))

        def rows(n):
            return pltpu.VMEM((3 * grps * n, 1, BLOCK), f32)

        def tiles(n, height=SUB):
            return pltpu.VMEM((n, height, BLOCK), f32)

        kinds = 1 + 2 * ITERS
        results = pl.pallas_call(
            functools.partial(body, (cells, grps, na, ng, nb, nq, nm)),
            out_shape=outs,
            in_specs=[hbm] * 10,
            out_specs=(vmem, vmem),
            scratch_shapes=[pltpu.SMEM(x.shape, x.dtype) for x in args[:3]]
            + [pltpu.VMEM(x.shape, x.dtype) for x in args[3:]]
            + [rows(3 * na), rows(4 * ng)]
            + [rows(3 * na) for _ in range(ITERS)]
            + [rows(ng) for _ in range(ITERS - 1)]
            + [pltpu.VMEM((cells * grps, 1, BLOCK), f32) for _ in range(ITERS)]
            + [
                pltpu.VMEM((na, 3, BLOCK, BLOCK), f32),
                pltpu.VMEM((ng, 3, BLOCK, BLOCK), f32),
                tiles(na * GROUPS * nb * 4),
                tiles(na * GROUPS * 4),
                tiles(na * GROUPS * nq * 3),
                tiles(ng * GROUPS * nm * 3),
                tiles(na * 5, cells),
                tiles(ng * 5, cells),
                tiles(na * GROUPS * 3),
                tiles(ng * GROUPS),
                dma((10,)),
                dma((kinds, 3 * grps)),
                dma((kinds, 3 * grps)),
                dma((ITERS,)),
                dma((ITERS,)),
            ],
            compiler_params=pltpu.CompilerParams(
                collective_id=0, has_side_effects=True, vmem_limit_bytes=40 << 20
            ),
        )(*args)
        return pl.pallas_call(
            hand_over,
            out_shape=outs,
            in_specs=[vmem, vmem],
            out_specs=(hbm, hbm),
            scratch_shapes=[dma((2,))],
            compiler_params=pltpu.CompilerParams(vmem_limit_bytes=1 << 20),
        )(*results)

    pair = P(("cell", "grp"))
    wide = P(None, ("cell", "grp"))
    tall = P(("cell", "grp"), None)
    return jax.shard_map(
        step,
        mesh=mesh,
        in_specs=(wide, wide, wide, wide, pair, pair, pair, tall, tall, tall),
        out_specs=(wide, pair),
        check_vma=False,
    )
```

```python
import functools
import math

import jax
import jax.numpy as jnp
from jax import lax
from jax.experimental import pallas as pl
from jax.experimental.pallas import tpu as pltpu
from jax.sharding import PartitionSpec as P

BLOCK = 128
SUB = 8
GROUPS = BLOCK // SUB
UNROLL = 8
HALVES = GROUPS // UNROLL
ITERS = 3
MESH = pl.DeviceIdType.MESH

soften_sq = 0.04


def body(dims, *refs):
    cells, grps, na, ng, nb, nq, nm = dims
    args, (out_dip, out_q), held = refs[:10], refs[10:12], refs[12:22]
    near_s, grid_s, source_s, sites, points, guess, fixed, pol, base, resp = held
    sit, pts = refs[22:24]
    mus = refs[24 : 24 + ITERS]
    chg = (None,) + refs[24 + ITERS : 23 + 2 * ITERS]
    tab = refs[23 + 2 * ITERS : 23 + 3 * ITERS]
    rest = refs[23 + 3 * ITERS :]
    tgt_a, tgt_g, geo, sgeo, cgeo, pgeo, fgeo_a, fgeo_g, acc_a, acc_g = rest[:10]
    load_sem, send_sem, recv_sem, far_send, far_recv, upward, downward = rest[10:]
    cell = lax.axis_index("cell")
    grp = lax.axis_index("grp")
    has_prev = cell > 0
    has_next = cell < cells - 1
    has_prev2 = cell > 1
    has_next2 = cell < cells - 2
    own = grps + grp
    cell_f = cell.astype(jnp.float32)
    centre = (cell_f + 0.5, 0.5, 0.5)
    pieces = 3 * grps
    order = sorted(range(grps), key=lambda d: (abs(2 * d - grps), d))

    site_msg = (sit, 3 * na, 0)
    point_msg = (pts, 4 * ng, 1)
    mu_msg = [(mus[it], 3 * na, 2 + it) for it in range(ITERS)]
    charge_msg = [None] + [(chg[it], ng, 1 + ITERS + it) for it in range(1, ITERS)]

    def vec_row(ref, a, b):
        return ref[a : a + 1, b * BLOCK : (b + 1) * BLOCK]

    def flat_row(ref, b):
        return ref[b * BLOCK : (b + 1) * BLOCK].reshape(1, BLOCK)

    lanes = lax.broadcasted_iota(jnp.int32, (SUB, BLOCK), 1)
    subs = lax.broadcasted_iota(jnp.int32, (SUB, BLOCK), 0)
    diag = lanes - subs

    barrier = pltpu.get_barrier_semaphore()

    def greet(c, g):
        pl.semaphore_signal(barrier, inc=1, device_id=(c, g), device_id_type=MESH)

    def greet_near():
        @pl.when(has_prev2)
        def _():
            greet(cell - 2, grp)

        @pl.when(has_prev)
        def _():
            for d in order:
                greet(cell - 1, lax.rem(grp + d, grps))

        @pl.when(has_next)
        def _():
            for d in order:
                greet(cell + 1, lax.rem(grp + d, grps))

        for d in range(1, grps):
            greet(cell, lax.rem(grp + d, grps))

        @pl.when(has_next2)
        def _():
            greet(cell + 2, grp)

    def each_other_cell(act):
        def step(n, carry):
            c = lax.rem(cell + n, cells)
            for d in range(grps):
                act(c, lax.rem(grp + d, grps))
            return carry

        lax.fori_loop(1, cells, step, 0)

    loads = [
        pltpu.make_async_copy(src, dst, load_sem.at[n])
        for n, (src, dst) in enumerate(zip(args, held))
    ]
    for n in (3, 5, 4, 8, 0, 1, 2, 6, 7, 9):
        loads[n].start()
    greet_near()

    def clear(slot):
        for buf, rows, _ in [site_msg, point_msg] + mu_msg + charge_msg[1:]:
            buf[slot * grps * rows : (slot + 1) * grps * rows] = jnp.zeros((grps * rows, 1, BLOCK), jnp.float32)

    for it in range(ITERS):
        for g in range(grps):
            tab[it][g * cells + cell] = jnp.zeros((1, BLOCK), jnp.float32)
    pl.when(jnp.logical_not(has_prev))(lambda: clear(0))
    pl.when(jnp.logical_not(has_next))(lambda: clear(2))

    greeted = [(has_prev, grps), (has_next, grps), (has_prev2, 1), (has_next2, 1)]
    pl.semaphore_wait(barrier, grps - 1 + sum(n * met.astype(jnp.int32) for met, n in greeted))
    edge_up, edge_down = jnp.logical_not(has_prev2), jnp.logical_not(has_next2)

    @pl.when(jnp.logical_and(edge_up, has_next2))
    def _():
        pl.semaphore_signal(upward, inc=1, device_id=(cell + 2, grp), device_id_type=MESH)

    @pl.when(jnp.logical_and(edge_down, has_prev2))
    def _():
        pl.semaphore_signal(downward, inc=1, device_id=(cell - 2, grp), device_id_type=MESH)

    for n in (3, 5, 4, 8):
        loads[n].wait()

    for b in range(na):
        for a in range(3):
            sit[own * 3 * na + b * 3 + a] = vec_row(sites, a, b)
            mus[0][own * 3 * na + b * 3 + a] = vec_row(guess, a, b)
    for b in range(ng):
        for a in range(3):
            pts[own * 4 * ng + b * 4 + a] = vec_row(points, a, b)
        pts[own * 4 * ng + b * 4 + 3] = flat_row(base, b)

    def inverse_of(dx, dy, dz):
        return lax.rsqrt(dx * dx + dy * dy + dz * dz + soften_sq)

    def store_dipole_pair(ref, slot, targets, source, self_mask):
        dx, dy, dz = (t - s for t, s in zip(targets, source))
        inv = inverse_of(dx, dy, dz)
        cube = inv * inv * inv
        weight = cube * lax.rsqrt(inv) * math.sqrt(3.0)
        ref[slot] = dx * weight
        ref[slot + 1] = dy * weight
        ref[slot + 2] = dz * weight
        ref[slot + 3] = cube if self_mask is None else jnp.where(self_mask, 0.0, cube)

    def store_charge_pair(ref, slot, targets, source):
        dx, dy, dz = (t - s for t, s in zip(targets, source))
        inv = inverse_of(dx, dy, dz)
        cube = inv * inv * inv
        ref[slot] = dx * cube
        ref[slot + 1] = dy * cube
        ref[slot + 2] = dz * cube

    def column_sum(x):
        return jnp.sum(x, axis=0, keepdims=True)

    def wide(row):
        return jnp.broadcast_to(row, (SUB, BLOCK))

    def targets_of(ref, b, group):
        return [ref[b, a, pl.ds(group * SUB, SUB), :] for a in range(3)]

    def piece_copy(msg, slot, c, g):
        buf, rows, kind = msg
        return pltpu.make_async_remote_copy(
            src_ref=buf.at[pl.ds(own * rows, rows)],
            dst_ref=buf.at[pl.ds((slot * grps + grp) * rows, rows)],
            send_sem=send_sem.at[kind, slot * grps + g],
            recv_sem=recv_sem.at[kind, slot * grps + grp],
            device_id=(c, g),
            device_id_type=MESH,
        )

    def for_all(msg, act):
        @pl.when(has_prev)
        def _():
            for d in order:
                g = lax.rem(grp + d, grps)
                act(piece_copy(msg, 2, cell - 1, g))

        @pl.when(has_next)
        def _():
            for d in order:
                g = lax.rem(grp + d, grps)
                act(piece_copy(msg, 0, cell + 1, g))

        for d in order:
            if d:
                g = lax.rem(grp + d, grps)
                act(piece_copy(msg, 1, cell, g))

    def arrival(msg, p, c, g):
        buf, rows, kind = msg
        pltpu.make_async_remote_copy(
            src_ref=buf.at[pl.ds(p * rows, rows)],
            dst_ref=buf.at[pl.ds(p * rows, rows)],
            send_sem=send_sem.at[kind, p],
            recv_sem=recv_sem.at[kind, p],
            device_id=(c, g),
            device_id_type=MESH,
        ).wait_recv()

    def all_arrive(msg):
        for d in range(1, grps):
            g = lax.rem(grp + d, grps)
            arrival(msg, grps + g, cell, g)

        @pl.when(has_prev)
        def _():
            for g in range(grps):
                arrival(msg, g, cell - 1, g)

        @pl.when(has_next)
        def _():
            for g in range(grps):
                arrival(msg, 2 * grps + g, cell + 1, g)

    def start(copy):
        copy.start()

    def finish(copy):
        copy.wait_send()

    def far_row(it, c, g):
        return tab[it].at[pl.ds(g * cells + c, 1)]

    def far_copy(it, c, g):
        return pltpu.make_async_remote_copy(
            src_ref=far_row(it, cell, grp),
            dst_ref=far_row(it, cell, grp),
            send_sem=far_send.at[it],
            recv_sem=far_recv.at[it],
            device_id=(c, g),
            device_id_type=MESH,
        )

    def far_all(it):
        rows = tab[it].at[pl.ds(0, (cells - 1) * grps)]
        return pltpu.make_async_remote_copy(
            src_ref=rows,
            dst_ref=rows,
            send_sem=far_send.at[it],
            recv_sem=far_recv.at[it],
            device_id=(lax.rem(cell + 1, cells), grp),
            device_id_type=MESH,
        )

    def charge_row(it, w):
        return pts[w * 4 + 3] if it == 0 else chg[it][w]

    def own_sums(it):
        rows = []
        for a in range(3):
            total = mus[it][own * 3 * na + a]
            for b in range(1, na):
                total = total + mus[it][own * 3 * na + b * 3 + a]
            rows.append(total)
        q = [charge_row(it, own * ng + b) for b in range(ng)]
        rows.append(functools.reduce(jnp.add, q))
        for a in range(3):
            rows.append(functools.reduce(jnp.add, [q[b] * (vec_row(points, a, b) - centre[a]) for b in range(ng)]))
        tile = jnp.zeros((SUB, BLOCK), jnp.float32)
        for n, row in enumerate(rows):
            tile = jnp.where(subs == n, wide(row), tile)
        sums = jnp.sum(tile, axis=1, keepdims=True)
        tab[it][grp * cells + cell] = column_sum(jnp.where(diag == 0, sums, 0.0))

    def far_sums(it):
        total = tab[it][0:cells, 0, :]
        for g in range(1, grps):
            total = total + tab[it][g * cells : (g + 1) * cells, 0, :]
        return [jnp.broadcast_to(total[:, n : n + 1], (cells, BLOCK)) for n in range(7)]

    def site_rows(w):
        return [wide(sit[w * 3 + a]) for a in range(3)]

    def point_rows(w):
        return [wide(pts[w * 4 + a]) for a in range(3)]

    def mu_rows(it, w):
        return [wide(mus[it][w * 3 + a]) for a in range(3)]

    def near_geometry(i, carry):
        b = lax.div(i, HALVES)
        first = lax.rem(i, HALVES) * UNROLL
        for k in range(nb):
            source = site_rows(near_s[b, k])
            for t in range(UNROLL):
                slot = ((i * UNROLL + t) * nb + k) * 4
                store_dipole_pair(geo, slot, targets_of(tgt_a, b, first + t), source, None)
        return carry

    def charge_geometry(i, carry):
        b = lax.div(i, HALVES)
        first = lax.rem(i, HALVES) * UNROLL
        for k in range(nq):
            source = point_rows(grid_s[b, k])
            for t in range(UNROLL):
                slot = ((i * UNROLL + t) * nq + k) * 3
                store_charge_pair(cgeo, slot, targets_of(tgt_a, b, first + t), source)
        return carry

    def grid_geometry(i, carry):
        b = lax.div(i, HALVES)
        first = lax.rem(i, HALVES) * UNROLL
        for k in range(nm):
            source = site_rows(source_s[b, k])
            for t in range(UNROLL):
                slot = ((i * UNROLL + t) * nm + k) * 3
                store_charge_pair(pgeo, slot, targets_of(tgt_g, b, first + t), source)
        return carry

    def self_atoms(it, i, carry):
        b = lax.div(i, HALVES)
        mu = mu_rows(it, own * na + b)
        for t in range(UNROLL):
            slot = (i * UNROLL + t) * 4
            u = [sgeo[slot + a] for a in range(3)]
            cube = sgeo[slot + 3]
            proj = u[0] * mu[0] + u[1] * mu[1] + u[2] * mu[2]
            for a in range(3):
                acc_a[(i * UNROLL + t) * 3 + a] = u[a] * proj - cube * mu[a]
        return carry

    def near_atoms(it, i, carry):
        b = lax.div(i, HALVES)
        acc = [[acc_a[(i * UNROLL + t) * 3 + a] for a in range(3)] for t in range(UNROLL)]
        for k in range(nb):
            mu = mu_rows(it, near_s[b, k])
            for t in range(UNROLL):
                slot = ((i * UNROLL + t) * nb + k) * 4
                u = [geo[slot + a] for a in range(3)]
                cube = geo[slot + 3]
                proj = u[0] * mu[0] + u[1] * mu[1] + u[2] * mu[2]
                for a in range(3):
                    acc[t][a] = acc[t][a] + (u[a] * proj - cube * mu[a])
        for t in range(UNROLL):
            for a in range(3):
                acc_a[(i * UNROLL + t) * 3 + a] = acc[t][a]
        return carry

    def near_grid(it, i, carry):
        b = lax.div(i, HALVES)
        acc = [None] * UNROLL
        for k in range(nm):
            mu = mu_rows(it, source_s[b, k])
            for t in range(UNROLL):
                slot = ((i * UNROLL + t) * nm + k) * 3
                term = pgeo[slot] * mu[0] + pgeo[slot + 1] * mu[1] + pgeo[slot + 2] * mu[2]
                acc[t] = term if k == 0 else acc[t] + term
        for t in range(UNROLL):
            acc_g[i * UNROLL + t] = acc[t]
        return carry

    def gather_lanes(tiles):
        row = jnp.zeros((SUB, BLOCK), jnp.float32)
        for t, tile in enumerate(tiles):
            total = jnp.sum(tile, axis=1, keepdims=True)
            row = jnp.where(diag == t * SUB, total, row)
        return column_sum(row)

    def atom_fields(it):
        rows = []
        for b in range(na):
            q = [wide(charge_row(it, grid_s[b, k])) for k in range(nq)]
            tiles = [[], [], []]
            for t in range(GROUPS):
                n = b * GROUPS + t
                for a in range(3):
                    terms = [cgeo[(n * nq + k) * 3 + a] * q[k] for k in range(nq)]
                    tiles[a].append(acc_a[n * 3 + a] + functools.reduce(jnp.add, terms))
            rows.append([gather_lanes(tiles[a]) for a in range(3)])
        return rows

    def grid_fields():
        return [gather_lanes([acc_g[b * GROUPS + t] for t in range(GROUPS)]) for b in range(ng)]

    def store_far(ref, n, row_of):
        c = lax.broadcasted_iota(jnp.int32, (cells, BLOCK), 0)
        dx = row_of(0) - (c.astype(jnp.float32) + 0.5)
        dy = jnp.broadcast_to(row_of(1) - 0.5, (cells, BLOCK))
        dz = jnp.broadcast_to(row_of(2) - 0.5, (cells, BLOCK))
        inv = inverse_of(dx, dy, dz)
        cube = jnp.where(jnp.abs(c - cell) >= 2, inv * inv * inv, 0.0)
        for m, x in enumerate((dx, dy, dz, cube, cube * inv * inv * 3.0)):
            ref[n * 5 + m] = x

    def finish_atoms(it, near, sums):
        moments = [sums[a] + sums[4 + a] for a in range(3)]
        for b in range(na):
            delta = [fgeo_a[b * 5 + a] for a in range(3)]
            cube, fifth = fgeo_a[b * 5 + 3], fgeo_a[b * 5 + 4]
            radial = fifth * (moments[0] * delta[0] + moments[1] * delta[1] + moments[2] * delta[2])
            radial = radial + sums[3] * cube
            for a in range(3):
                far = column_sum(radial * delta[a] - moments[a] * cube)
                new = flat_row(pol, b) * (vec_row(fixed, a, b) + (near[b][a] + far))
                if it + 1 < ITERS:
                    mus[it + 1][own * 3 * na + b * 3 + a] = new
                else:
                    out_dip[a : a + 1, b * BLOCK : (b + 1) * BLOCK] = new

    def finish_grid(it, near, sums):
        for b in range(ng):
            delta = [fgeo_g[b * 5 + a] for a in range(3)]
            proj = sums[0] * delta[0] + sums[1] * delta[1] + sums[2] * delta[2]
            far = column_sum(proj * fgeo_g[b * 5 + 3])
            new = flat_row(base, b) - flat_row(resp, b) * (near[b] + far)
            if it + 1 < ITERS:
                chg[it + 1][own * ng + b] = new
            else:
                out_q[b * BLOCK : (b + 1) * BLOCK] = new.reshape(BLOCK)

    atom_steps, grid_steps = na * HALVES, ng * HALVES

    for_all(site_msg, start)
    for_all(mu_msg[0], start)
    for_all(point_msg, start)
    own_sums(0)

    @pl.when(has_prev2)
    def _():
        pl.semaphore_wait(upward, 1)

    @pl.when(jnp.logical_and(has_prev2, has_next2))
    def _():
        pl.semaphore_signal(upward, inc=1, device_id=(cell + 2, grp), device_id_type=MESH)

    @pl.when(has_next2)
    def _():
        pl.semaphore_wait(downward, 1)

    @pl.when(jnp.logical_and(has_prev2, has_next2))
    def _():
        pl.semaphore_signal(downward, inc=1, device_id=(cell - 2, grp), device_id_type=MESH)

    each_other_cell(lambda c, g: far_copy(0, c, g).start())

    for a in range(3):
        for b in range(na):
            tgt_a[b, a] = jnp.transpose(jnp.broadcast_to(vec_row(sites, a, b), (BLOCK, BLOCK)))
        for b in range(ng):
            tgt_g[b, a] = jnp.transpose(jnp.broadcast_to(vec_row(points, a, b), (BLOCK, BLOCK)))
    for b in range(na):
        source = [wide(vec_row(sites, a, b)) for a in range(3)]
        for t in range(GROUPS):
            store_dipole_pair(sgeo, (b * GROUPS + t) * 4, targets_of(tgt_a, b, t), source, diag == t * SUB)
    lax.fori_loop(0, atom_steps, functools.partial(self_atoms, 0), 0)
    for b in range(na):
        store_far(fgeo_a, b, lambda a: vec_row(sites, a, b))
    for b in range(ng):
        store_far(fgeo_g, b, lambda a: vec_row(points, a, b))
    for n in (0, 1, 2, 6, 7, 9):
        loads[n].wait()

    all_arrive(site_msg)
    lax.fori_loop(0, atom_steps, near_geometry, 0)

    for it in range(ITERS):
        last = it + 1 == ITERS
        all_arrive(mu_msg[it])
        lax.fori_loop(0, atom_steps, functools.partial(near_atoms, it), 0)
        if last:
            lax.fori_loop(0, grid_steps, functools.partial(near_grid, it), 0)
        if it == 0:
            all_arrive(point_msg)
            lax.fori_loop(0, atom_steps, charge_geometry, 0)
        else:
            all_arrive(charge_msg[it])
        far_all(it).wait_recv()
        sums = far_sums(it)
        finish_atoms(it, atom_fields(it), sums)
        if last:
            finish_grid(it, grid_fields(), sums)
            break
        for_all(mu_msg[it + 1], start)
        if it == 0:
            lax.fori_loop(0, grid_steps, grid_geometry, 0)
        lax.fori_loop(0, grid_steps, functools.partial(near_grid, it), 0)
        finish_grid(it, grid_fields(), sums)
        for_all(charge_msg[it + 1], start)
        own_sums(it + 1)
        each_other_cell(lambda c, g: far_copy(it + 1, c, g).start())
        lax.fori_loop(0, atom_steps, functools.partial(self_atoms, it + 1), 0)

    for msg in [site_msg, point_msg] + mu_msg + charge_msg[1:]:
        for_all(msg, finish)
    for it in range(ITERS):
        far_all(it).wait_send()


def hand_over(dip, q, out_dip, out_q, sem):
    copies = [
        pltpu.make_async_copy(dip, out_dip, sem.at[0]),
        pltpu.make_async_copy(q, out_q, sem.at[1]),
    ]
    for copy in copies:
        copy.start()
    for copy in copies:
        copy.wait()


def solution(mesh):
    cells, grps = mesh.shape["cell"], mesh.shape["grp"]

    def step(sites, points, guess, fixed, pol, base, resp, near, grid, source):
        na, nb = near.shape
        nq = grid.shape[1]
        ng, nm = source.shape
        f32 = jnp.float32
        args = (near, grid, source, sites, points, guess, fixed, pol, base, resp)
        args = tuple(pltpu.with_memory_space_constraint(x, pltpu.HBM) for x in args)
        vmem = pl.BlockSpec(memory_space=pltpu.VMEM)
        hbm = pl.BlockSpec(memory_space=pltpu.HBM)
        dma = pltpu.SemaphoreType.DMA
        outs = (jax.ShapeDtypeStruct(sites.shape, f32), jax.ShapeDtypeStruct(base.shape, f32))

        def rows(n):
            return pltpu.VMEM((3 * grps * n, 1, BLOCK), f32)

        def tiles(n, height=SUB):
            return pltpu.VMEM((n, height, BLOCK), f32)

        kinds = 1 + 2 * ITERS
        results = pl.pallas_call(
            functools.partial(body, (cells, grps, na, ng, nb, nq, nm)),
            out_shape=outs,
            in_specs=[hbm] * 10,
            out_specs=(vmem, vmem),
            scratch_shapes=[pltpu.SMEM(x.shape, x.dtype) for x in args[:3]]
            + [pltpu.VMEM(x.shape, x.dtype) for x in args[3:]]
            + [rows(3 * na), rows(4 * ng)]
            + [rows(3 * na) for _ in range(ITERS)]
            + [rows(ng) for _ in range(ITERS - 1)]
            + [pltpu.VMEM((cells * grps, 1, BLOCK), f32) for _ in range(ITERS)]
            + [
                pltpu.VMEM((na, 3, BLOCK, BLOCK), f32),
                pltpu.VMEM((ng, 3, BLOCK, BLOCK), f32),
                tiles(na * GROUPS * nb * 4),
                tiles(na * GROUPS * 4),
                tiles(na * GROUPS * nq * 3),
                tiles(ng * GROUPS * nm * 3),
                tiles(na * 5, cells),
                tiles(ng * 5, cells),
                tiles(na * GROUPS * 3),
                tiles(ng * GROUPS),
                dma((10,)),
                dma((kinds, 3 * grps)),
                dma((kinds, 3 * grps)),
                dma((ITERS,)),
                dma((ITERS,)),
                pltpu.SemaphoreType.REGULAR,
                pltpu.SemaphoreType.REGULAR,
            ],
            compiler_params=pltpu.CompilerParams(
                collective_id=0, has_side_effects=True, vmem_limit_bytes=40 << 20
            ),
        )(*args)
        return pl.pallas_call(
            hand_over,
            out_shape=outs,
            in_specs=[vmem, vmem],
            out_specs=(hbm, hbm),
            scratch_shapes=[dma((2,))],
            compiler_params=pltpu.CompilerParams(vmem_limit_bytes=1 << 20),
        )(*results)

    pair = P(("cell", "grp"))
    wide = P(None, ("cell", "grp"))
    tall = P(("cell", "grp"), None)
    return jax.shard_map(
        step,
        mesh=mesh,
        in_specs=(wide, wide, wide, wide, pair, pair, pair, tall, tall, tall),
        out_specs=(wide, pair),
        check_vma=False,
    )
```

```python
import functools
import math

import jax
import jax.numpy as jnp
from jax import lax
from jax.experimental import pallas as pl
from jax.experimental.pallas import tpu as pltpu
from jax.sharding import PartitionSpec as P

BLOCK = 128
SUB = 8
GROUPS = BLOCK // SUB
UNROLL = 8
HALVES = GROUPS // UNROLL
ITERS = 3
MESH = pl.DeviceIdType.MESH

soften_sq = 0.04


def body(dims, *refs):
    cells, grps, na, ng, nb, nq, nm = dims
    args, (out_dip, out_q), held = refs[:10], refs[10:12], refs[12:22]
    near_s, grid_s, source_s, sites, points, guess, fixed, pol, base, resp = held
    sit, pts = refs[22:24]
    mus = refs[24 : 24 + ITERS]
    chg = (None,) + refs[24 + ITERS : 23 + 2 * ITERS]
    tab = refs[23 + 2 * ITERS : 23 + 3 * ITERS]
    rest = refs[23 + 3 * ITERS :]
    tgt_a, tgt_g, geo, sgeo, cgeo, pgeo, fgeo_a, fgeo_g, acc_a, acc_g = rest[:10]
    load_sem, send_sem, recv_sem, far_send, far_recv, upward, downward = rest[10:]
    cell = lax.axis_index("cell")
    grp = lax.axis_index("grp")
    has_prev = cell > 0
    has_next = cell < cells - 1
    has_prev2 = cell > 1
    has_next2 = cell < cells - 2
    own = grps + grp
    cell_f = cell.astype(jnp.float32)
    centre = (cell_f + 0.5, 0.5, 0.5)
    pieces = 3 * grps
    order = sorted(range(grps), key=lambda d: (abs(2 * d - grps), d))

    site_msg = (sit, 3 * na, 0)
    point_msg = (pts, 4 * ng, 1)
    mu_msg = [(mus[it], 3 * na, 2 + it) for it in range(ITERS)]
    charge_msg = [None] + [(chg[it], ng, 1 + ITERS + it) for it in range(1, ITERS)]

    def vec_row(ref, a, b):
        return ref[a : a + 1, b * BLOCK : (b + 1) * BLOCK]

    def flat_row(ref, b):
        return ref[b * BLOCK : (b + 1) * BLOCK].reshape(1, BLOCK)

    lanes = lax.broadcasted_iota(jnp.int32, (SUB, BLOCK), 1)
    subs = lax.broadcasted_iota(jnp.int32, (SUB, BLOCK), 0)
    diag = lanes - subs

    barrier = pltpu.get_barrier_semaphore()

    def greet(c, g):
        pl.semaphore_signal(barrier, inc=1, device_id=(c, g), device_id_type=MESH)

    def greet_near():
        @pl.when(has_prev2)
        def _():
            greet(cell - 2, grp)

        @pl.when(has_prev)
        def _():
            for d in order:
                greet(cell - 1, lax.rem(grp + d, grps))

        @pl.when(has_next)
        def _():
            for d in order:
                greet(cell + 1, lax.rem(grp + d, grps))

        for d in range(1, grps):
            greet(cell, lax.rem(grp + d, grps))

        @pl.when(has_next2)
        def _():
            greet(cell + 2, grp)

    def each_far_cell(act):
        def step(c, carry):
            for d in order:
                act(c, lax.rem(grp + d, grps))
            return carry

        lax.fori_loop(0, cell - 1, step, 0)
        lax.fori_loop(0, cells - 2 - cell, lambda n, carry: step(cells - 1 - n, carry), 0)

    loads = [
        pltpu.make_async_copy(src, dst, load_sem.at[n])
        for n, (src, dst) in enumerate(zip(args, held))
    ]
    for n in (3, 5, 4, 8, 0, 1, 2, 6, 7, 9):
        loads[n].start()
    greet_near()

    def clear(slot):
        for buf, rows, _ in [site_msg, point_msg] + mu_msg + charge_msg[1:]:
            buf[slot * grps * rows : (slot + 1) * grps * rows] = jnp.zeros((grps * rows, 1, BLOCK), jnp.float32)

    for it in range(ITERS):
        for g in range(grps):
            for c in (lax.max(cell - 1, 0), cell, lax.min(cell + 1, cells - 1)):
                tab[it][g * cells + c] = jnp.zeros((1, BLOCK), jnp.float32)
    pl.when(jnp.logical_not(has_prev))(lambda: clear(0))
    pl.when(jnp.logical_not(has_next))(lambda: clear(2))

    greeted = [(has_prev, grps), (has_next, grps), (has_prev2, 1), (has_next2, 1)]
    pl.semaphore_wait(barrier, grps - 1 + sum(n * met.astype(jnp.int32) for met, n in greeted))
    edge_up, edge_down = jnp.logical_not(has_prev2), jnp.logical_not(has_next2)

    @pl.when(jnp.logical_and(edge_up, has_next2))
    def _():
        pl.semaphore_signal(upward, inc=1, device_id=(cell + 2, grp), device_id_type=MESH)

    @pl.when(jnp.logical_and(edge_down, has_prev2))
    def _():
        pl.semaphore_signal(downward, inc=1, device_id=(cell - 2, grp), device_id_type=MESH)

    for n in (3, 5, 4, 8):
        loads[n].wait()

    for b in range(na):
        for a in range(3):
            sit[own * 3 * na + b * 3 + a] = vec_row(sites, a, b)
            mus[0][own * 3 * na + b * 3 + a] = vec_row(guess, a, b)
    for b in range(ng):
        for a in range(3):
            pts[own * 4 * ng + b * 4 + a] = vec_row(points, a, b)
        pts[own * 4 * ng + b * 4 + 3] = flat_row(base, b)

    def inverse_of(dx, dy, dz):
        return lax.rsqrt(dx * dx + dy * dy + dz * dz + soften_sq)

    def store_dipole_pair(ref, slot, targets, source, self_mask):
        dx, dy, dz = (t - s for t, s in zip(targets, source))
        inv = inverse_of(dx, dy, dz)
        cube = inv * inv * inv
        weight = inv * math.sqrt(3.0)
        ref[slot] = dx * weight
        ref[slot + 1] = dy * weight
        ref[slot + 2] = dz * weight
        ref[slot + 3] = cube if self_mask is None else jnp.where(self_mask, 0.0, cube)

    def store_charge_pair(ref, slot, targets, source):
        dx, dy, dz = (t - s for t, s in zip(targets, source))
        inv = inverse_of(dx, dy, dz)
        cube = inv * inv * inv
        ref[slot] = dx * cube
        ref[slot + 1] = dy * cube
        ref[slot + 2] = dz * cube

    def column_sum(x):
        return jnp.sum(x, axis=0, keepdims=True)

    def wide(row):
        return jnp.broadcast_to(row, (SUB, BLOCK))

    def targets_of(ref, b, group):
        return [ref[b, a, pl.ds(group * SUB, SUB), :] for a in range(3)]

    def piece_copy(msg, slot, c, g):
        buf, rows, kind = msg
        return pltpu.make_async_remote_copy(
            src_ref=buf.at[pl.ds(own * rows, rows)],
            dst_ref=buf.at[pl.ds((slot * grps + grp) * rows, rows)],
            send_sem=send_sem.at[kind],
            recv_sem=recv_sem.at[kind],
            device_id=(c, g),
            device_id_type=MESH,
        )

    def for_all(msg, act):
        @pl.when(has_prev)
        def _():
            for d in order:
                g = lax.rem(grp + d, grps)
                act(piece_copy(msg, 2, cell - 1, g))

        @pl.when(has_next)
        def _():
            for d in order:
                g = lax.rem(grp + d, grps)
                act(piece_copy(msg, 0, cell + 1, g))

        for d in order:
            if d:
                g = lax.rem(grp + d, grps)
                act(piece_copy(msg, 1, cell, g))

    inner = jnp.logical_and(has_prev, has_next)

    def traffic(msg, act):
        buf, rows, kind = msg

        def part(n):
            some = buf.at[pl.ds(0, n * rows)]
            act(
                pltpu.make_async_remote_copy(
                    src_ref=some,
                    dst_ref=some,
                    send_sem=send_sem.at[kind],
                    recv_sem=recv_sem.at[kind],
                    device_id=(cell, lax.rem(grp + 1, grps)),
                    device_id_type=MESH,
                )
            )

        pl.when(inner)(lambda: part(3 * grps - 1))
        pl.when(jnp.logical_not(inner))(lambda: part(2 * grps - 1))

    def all_arrive(msg):
        traffic(msg, arrive)

    def start(copy):
        copy.start()

    def arrive(copy):
        copy.wait_recv()

    def finish(copy):
        copy.wait_send()

    def far_row(it, c, g):
        return tab[it].at[pl.ds(g * cells + c, 1)]

    def far_copy(it, c, g):
        return pltpu.make_async_remote_copy(
            src_ref=far_row(it, cell, grp),
            dst_ref=far_row(it, cell, grp),
            send_sem=far_send.at[it],
            recv_sem=far_recv.at[it],
            device_id=(c, g),
            device_id_type=MESH,
        )

    def far_all(it, act):
        pl.when(inner)(lambda: act(far_rows(it, cells - 3)))
        pl.when(jnp.logical_not(inner))(lambda: act(far_rows(it, cells - 2)))

    def far_rows(it, n):
        rows = tab[it].at[pl.ds(0, n * grps)]
        return pltpu.make_async_remote_copy(
            src_ref=rows,
            dst_ref=rows,
            send_sem=far_send.at[it],
            recv_sem=far_recv.at[it],
            device_id=(lax.rem(cell + 1, cells), grp),
            device_id_type=MESH,
        )

    def charge_row(it, w):
        return pts[w * 4 + 3] if it == 0 else chg[it][w]

    def own_sums(it):
        rows = []
        for a in range(3):
            total = mus[it][own * 3 * na + a]
            for b in range(1, na):
                total = total + mus[it][own * 3 * na + b * 3 + a]
            rows.append(total)
        q = [charge_row(it, own * ng + b) for b in range(ng)]
        rows.append(functools.reduce(jnp.add, q))
        for a in range(3):
            rows.append(functools.reduce(jnp.add, [q[b] * (vec_row(points, a, b) - centre[a]) for b in range(ng)]))
        tile = jnp.zeros((SUB, BLOCK), jnp.float32)
        for n, row in enumerate(rows):
            tile = jnp.where(subs == n, wide(row), tile)
        sums = jnp.sum(tile, axis=1, keepdims=True)
        tab[it][grp * cells + cell] = column_sum(jnp.where(diag == 0, sums, 0.0))

    def far_sums(it):
        total = tab[it][0:cells, 0, :]
        for g in range(1, grps):
            total = total + tab[it][g * cells : (g + 1) * cells, 0, :]
        return [jnp.broadcast_to(total[:, n : n + 1], (cells, BLOCK)) for n in range(7)]

    def site_rows(w):
        return [wide(sit[w * 3 + a]) for a in range(3)]

    def point_rows(w):
        return [wide(pts[w * 4 + a]) for a in range(3)]

    def mu_rows(it, w):
        return [wide(mus[it][w * 3 + a]) for a in range(3)]

    def near_geometry(i, carry):
        b = lax.div(i, HALVES)
        first = lax.rem(i, HALVES) * UNROLL
        for k in range(nb):
            source = site_rows(near_s[b, k])
            for t in range(UNROLL):
                slot = ((i * UNROLL + t) * nb + k) * 4
                store_dipole_pair(geo, slot, targets_of(tgt_a, b, first + t), source, None)
        return carry

    def charge_geometry(i, carry):
        b = lax.div(i, HALVES)
        first = lax.rem(i, HALVES) * UNROLL
        for k in range(nq):
            source = point_rows(grid_s[b, k])
            for t in range(UNROLL):
                slot = ((i * UNROLL + t) * nq + k) * 3
                store_charge_pair(cgeo, slot, targets_of(tgt_a, b, first + t), source)
        return carry

    def grid_geometry(i, carry):
        b = lax.div(i, HALVES)
        first = lax.rem(i, HALVES) * UNROLL
        for k in range(nm):
            source = site_rows(source_s[b, k])
            for t in range(UNROLL):
                slot = ((i * UNROLL + t) * nm + k) * 3
                store_charge_pair(pgeo, slot, targets_of(tgt_g, b, first + t), source)
        return carry

    def self_atoms(it, i, carry):
        b = lax.div(i, HALVES)
        mu = mu_rows(it, own * na + b)
        for t in range(UNROLL):
            slot = (i * UNROLL + t) * 4
            u = [sgeo[slot + a] for a in range(3)]
            cube = sgeo[slot + 3]
            proj = u[0] * mu[0] + u[1] * mu[1] + u[2] * mu[2]
            for a in range(3):
                acc_a[(i * UNROLL + t) * 3 + a] = cube * (u[a] * proj - mu[a])
        return carry

    def near_atoms(it, i, carry):
        b = lax.div(i, HALVES)
        acc = [[acc_a[(i * UNROLL + t) * 3 + a] for a in range(3)] for t in range(UNROLL)]
        for k in range(nb):
            mu = mu_rows(it, near_s[b, k])
            for t in range(UNROLL):
                slot = ((i * UNROLL + t) * nb + k) * 4
                u = [geo[slot + a] for a in range(3)]
                cube = geo[slot + 3]
                proj = u[0] * mu[0] + u[1] * mu[1] + u[2] * mu[2]
                for a in range(3):
                    acc[t][a] = acc[t][a] + cube * (u[a] * proj - mu[a])
        for t in range(UNROLL):
            for a in range(3):
                acc_a[(i * UNROLL + t) * 3 + a] = acc[t][a]
        return carry

    def near_grid(it, i, carry):
        b = lax.div(i, HALVES)
        acc = [None] * UNROLL
        for k in range(nm):
            mu = mu_rows(it, source_s[b, k])
            for t in range(UNROLL):
                slot = ((i * UNROLL + t) * nm + k) * 3
                term = pgeo[slot] * mu[0] + pgeo[slot + 1] * mu[1] + pgeo[slot + 2] * mu[2]
                acc[t] = term if k == 0 else acc[t] + term
        for t in range(UNROLL):
            acc_g[i * UNROLL + t] = acc[t]
        return carry

    def gather_lanes(tiles):
        row = jnp.zeros((SUB, BLOCK), jnp.float32)
        for t, tile in enumerate(tiles):
            total = jnp.sum(tile, axis=1, keepdims=True)
            row = jnp.where(diag == t * SUB, total, row)
        return column_sum(row)

    def atom_fields(it):
        rows = []
        for b in range(na):
            q = [wide(charge_row(it, grid_s[b, k])) for k in range(nq)]
            tiles = [[], [], []]
            for t in range(GROUPS):
                n = b * GROUPS + t
                for a in range(3):
                    terms = [cgeo[(n * nq + k) * 3 + a] * q[k] for k in range(nq)]
                    tiles[a].append(acc_a[n * 3 + a] + functools.reduce(jnp.add, terms))
            rows.append([gather_lanes(tiles[a]) for a in range(3)])
        return rows

    def grid_fields():
        return [gather_lanes([acc_g[b * GROUPS + t] for t in range(GROUPS)]) for b in range(ng)]

    def store_far(ref, n, row_of):
        c = lax.broadcasted_iota(jnp.int32, (cells, BLOCK), 0)
        dx = row_of(0) - (c.astype(jnp.float32) + 0.5)
        dy = jnp.broadcast_to(row_of(1) - 0.5, (cells, BLOCK))
        dz = jnp.broadcast_to(row_of(2) - 0.5, (cells, BLOCK))
        inv = inverse_of(dx, dy, dz)
        cube = jnp.where(jnp.abs(c - cell) >= 2, inv * inv * inv, 0.0)
        for m, x in enumerate((dx, dy, dz, cube, cube * inv * inv * 3.0)):
            ref[n * 5 + m] = x

    def finish_atoms(it, near, sums):
        moments = [sums[a] + sums[4 + a] for a in range(3)]
        for b in range(na):
            delta = [fgeo_a[b * 5 + a] for a in range(3)]
            cube, fifth = fgeo_a[b * 5 + 3], fgeo_a[b * 5 + 4]
            radial = fifth * (moments[0] * delta[0] + moments[1] * delta[1] + moments[2] * delta[2])
            radial = radial + sums[3] * cube
            for a in range(3):
                far = column_sum(radial * delta[a] - moments[a] * cube)
                new = flat_row(pol, b) * (vec_row(fixed, a, b) + (near[b][a] + far))
                if it + 1 < ITERS:
                    mus[it + 1][own * 3 * na + b * 3 + a] = new
                else:
                    out_dip[a : a + 1, b * BLOCK : (b + 1) * BLOCK] = new

    def finish_grid(it, near, sums):
        for b in range(ng):
            delta = [fgeo_g[b * 5 + a] for a in range(3)]
            proj = sums[0] * delta[0] + sums[1] * delta[1] + sums[2] * delta[2]
            far = column_sum(proj * fgeo_g[b * 5 + 3])
            new = flat_row(base, b) - flat_row(resp, b) * (near[b] + far)
            if it + 1 < ITERS:
                chg[it + 1][own * ng + b] = new
            else:
                out_q[b * BLOCK : (b + 1) * BLOCK] = new.reshape(BLOCK)

    def repeat(n, chunk, fn):
        def step(j, carry):
            for m in range(chunk):
                fn(j * chunk + m, carry)
            return carry

        if chunk == n:
            step(0, 0)
        else:
            lax.fori_loop(0, n // chunk, step, 0)

    atom_steps, grid_steps = na * HALVES, ng * HALVES

    for_all(site_msg, start)
    for_all(mu_msg[0], start)
    for_all(point_msg, start)
    own_sums(0)

    @pl.when(has_prev2)
    def _():
        pl.semaphore_wait(upward, 1)

    @pl.when(jnp.logical_and(has_prev2, has_next2))
    def _():
        pl.semaphore_signal(upward, inc=1, device_id=(cell + 2, grp), device_id_type=MESH)

    @pl.when(has_next2)
    def _():
        pl.semaphore_wait(downward, 1)

    @pl.when(jnp.logical_and(has_prev2, has_next2))
    def _():
        pl.semaphore_signal(downward, inc=1, device_id=(cell - 2, grp), device_id_type=MESH)

    each_far_cell(lambda c, g: far_copy(0, c, g).start())

    for a in range(3):
        for b in range(na):
            tgt_a[b, a] = jnp.transpose(jnp.broadcast_to(vec_row(sites, a, b), (BLOCK, BLOCK)))
        for b in range(ng):
            tgt_g[b, a] = jnp.transpose(jnp.broadcast_to(vec_row(points, a, b), (BLOCK, BLOCK)))
    for b in range(na):
        source = [wide(vec_row(sites, a, b)) for a in range(3)]
        for t in range(GROUPS):
            store_dipole_pair(sgeo, (b * GROUPS + t) * 4, targets_of(tgt_a, b, t), source, diag == t * SUB)
    repeat(atom_steps, 4, functools.partial(self_atoms, 0))
    for b in range(na):
        store_far(fgeo_a, b, lambda a: vec_row(sites, a, b))
    for b in range(ng):
        store_far(fgeo_g, b, lambda a: vec_row(points, a, b))
    for n in (0, 1, 2, 6, 7, 9):
        loads[n].wait()

    all_arrive(site_msg)
    repeat(atom_steps, 4, near_geometry)

    for it in range(ITERS):
        last = it + 1 == ITERS
        all_arrive(mu_msg[it])
        repeat(atom_steps, 4, functools.partial(near_atoms, it))
        if it:
            repeat(grid_steps, 3, functools.partial(near_grid, it))
        if it == 0:
            all_arrive(point_msg)
            repeat(atom_steps, 4, charge_geometry)
        else:
            all_arrive(charge_msg[it])
        atom_near = atom_fields(it)
        grid_near = grid_fields() if it else None
        far_all(it, arrive)
        sums = far_sums(it)
        finish_atoms(it, atom_near, sums)
        if last:
            finish_grid(it, grid_near, sums)
            break
        for_all(mu_msg[it + 1], start)
        if it == 0:
            repeat(grid_steps, 3, grid_geometry)
            repeat(grid_steps, 3, functools.partial(near_grid, it))
            grid_near = grid_fields()
        finish_grid(it, grid_near, sums)
        own_sums(it + 1)
        each_far_cell(lambda c, g: far_copy(it + 1, c, g).start())
        for_all(charge_msg[it + 1], start)
        repeat(atom_steps, 4, functools.partial(self_atoms, it + 1))

    for msg in [site_msg, point_msg] + mu_msg + charge_msg[1:]:
        traffic(msg, finish)
    for it in range(ITERS):
        far_all(it, finish)


def hand_over(dip, q, out_dip, out_q, sem):
    copies = [
        pltpu.make_async_copy(dip, out_dip, sem.at[0]),
        pltpu.make_async_copy(q, out_q, sem.at[1]),
    ]
    for copy in copies:
        copy.start()
    for copy in copies:
        copy.wait()


def solution(mesh):
    cells, grps = mesh.shape["cell"], mesh.shape["grp"]

    def step(sites, points, guess, fixed, pol, base, resp, near, grid, source):
        na, nb = near.shape
        nq = grid.shape[1]
        ng, nm = source.shape
        f32 = jnp.float32
        args = (near, grid, source, sites, points, guess, fixed, pol, base, resp)
        args = tuple(pltpu.with_memory_space_constraint(x, pltpu.HBM) for x in args)
        vmem = pl.BlockSpec(memory_space=pltpu.VMEM)
        hbm = pl.BlockSpec(memory_space=pltpu.HBM)
        dma = pltpu.SemaphoreType.DMA
        outs = (jax.ShapeDtypeStruct(sites.shape, f32), jax.ShapeDtypeStruct(base.shape, f32))

        def rows(n):
            return pltpu.VMEM((3 * grps * n, 1, BLOCK), f32)

        def tiles(n, height=SUB):
            return pltpu.VMEM((n, height, BLOCK), f32)

        kinds = 1 + 2 * ITERS
        results = pl.pallas_call(
            functools.partial(body, (cells, grps, na, ng, nb, nq, nm)),
            out_shape=outs,
            in_specs=[hbm] * 10,
            out_specs=(vmem, vmem),
            scratch_shapes=[pltpu.SMEM(x.shape, x.dtype) for x in args[:3]]
            + [pltpu.VMEM(x.shape, x.dtype) for x in args[3:]]
            + [rows(3 * na), rows(4 * ng)]
            + [rows(3 * na) for _ in range(ITERS)]
            + [rows(ng) for _ in range(ITERS - 1)]
            + [pltpu.VMEM((cells * grps, 1, BLOCK), f32) for _ in range(ITERS)]
            + [
                pltpu.VMEM((na, 3, BLOCK, BLOCK), f32),
                pltpu.VMEM((ng, 3, BLOCK, BLOCK), f32),
                tiles(na * GROUPS * nb * 4),
                tiles(na * GROUPS * 4),
                tiles(na * GROUPS * nq * 3),
                tiles(ng * GROUPS * nm * 3),
                tiles(na * 5, cells),
                tiles(ng * 5, cells),
                tiles(na * GROUPS * 3),
                tiles(ng * GROUPS),
                dma((10,)),
                dma((kinds,)),
                dma((kinds,)),
                dma((ITERS,)),
                dma((ITERS,)),
                pltpu.SemaphoreType.REGULAR,
                pltpu.SemaphoreType.REGULAR,
            ],
            compiler_params=pltpu.CompilerParams(
                collective_id=0, has_side_effects=True, vmem_limit_bytes=40 << 20
            ),
        )(*args)
        return pl.pallas_call(
            hand_over,
            out_shape=outs,
            in_specs=[vmem, vmem],
            out_specs=(hbm, hbm),
            scratch_shapes=[dma((2,))],
            compiler_params=pltpu.CompilerParams(vmem_limit_bytes=1 << 20),
        )(*results)

    pair = P(("cell", "grp"))
    wide = P(None, ("cell", "grp"))
    tall = P(("cell", "grp"), None)
    return jax.shard_map(
        step,
        mesh=mesh,
        in_specs=(wide, wide, wide, wide, pair, pair, pair, tall, tall, tall),
        out_specs=(wide, pair),
        check_vma=False,
    )
```

```python
import functools
import math

import jax
import jax.numpy as jnp
from jax import lax
from jax.experimental import pallas as pl
from jax.experimental.pallas import tpu as pltpu
from jax.sharding import PartitionSpec as P

BLOCK = 128
SUB = 8
GROUPS = BLOCK // SUB
UNROLL = 8
HALVES = GROUPS // UNROLL
ITERS = 3
MESH = pl.DeviceIdType.MESH

soften_sq = 0.04


def body(dims, *refs):
    cells, grps, na, ng, nb, nq, nm = dims
    args, (out_dip, out_q), held = refs[:10], refs[10:12], refs[12:22]
    near_s, grid_s, source_s, sites, points, guess, fixed, pol, base, resp = held
    sit, pts = refs[22:24]
    mus = refs[24 : 24 + ITERS]
    chg = (None,) + refs[24 + ITERS : 23 + 2 * ITERS]
    tab = refs[23 + 2 * ITERS : 23 + 3 * ITERS]
    rest = refs[23 + 3 * ITERS :]
    tgt_a, tgt_g, geo, sgeo, cgeo, pgeo, fgeo_a, fgeo_g, acc_a, acc_g = rest[:10]
    load_sem, send_sem, recv_sem, far_send, far_recv, upward, downward = rest[10:]
    cell = lax.axis_index("cell")
    grp = lax.axis_index("grp")
    has_prev = cell > 0
    has_next = cell < cells - 1
    has_prev2 = cell > 1
    has_next2 = cell < cells - 2
    own = grps + grp
    cell_f = cell.astype(jnp.float32)
    centre = (cell_f + 0.5, 0.5, 0.5)
    pieces = 3 * grps
    order = sorted(range(grps), key=lambda d: (abs(2 * d - grps), d))

    site_msg = (sit, 3 * na, 0)
    point_msg = (pts, 4 * ng, 1)
    mu_msg = [(mus[it], 3 * na, 2 + it) for it in range(ITERS)]
    charge_msg = [None] + [(chg[it], ng, 1 + ITERS + it) for it in range(1, ITERS)]

    def vec_row(ref, a, b):
        return ref[a : a + 1, b * BLOCK : (b + 1) * BLOCK]

    def flat_row(ref, b):
        return ref[b * BLOCK : (b + 1) * BLOCK].reshape(1, BLOCK)

    lanes = lax.broadcasted_iota(jnp.int32, (SUB, BLOCK), 1)
    subs = lax.broadcasted_iota(jnp.int32, (SUB, BLOCK), 0)
    diag = lanes - subs

    barrier = pltpu.get_barrier_semaphore()

    def greet(c, g):
        pl.semaphore_signal(barrier, inc=1, device_id=(c, g), device_id_type=MESH)

    def greet_near():
        @pl.when(has_prev2)
        def _():
            greet(cell - 2, grp)

        @pl.when(has_prev)
        def _():
            for d in order:
                greet(cell - 1, lax.rem(grp + d, grps))

        @pl.when(has_next)
        def _():
            for d in order:
                greet(cell + 1, lax.rem(grp + d, grps))

        for d in range(1, grps):
            greet(cell, lax.rem(grp + d, grps))

        @pl.when(has_next2)
        def _():
            greet(cell + 2, grp)

    def each_far_cell(act):
        def step(c, carry):
            for d in order:
                act(c, lax.rem(grp + d, grps))
            return carry

        lax.fori_loop(0, cell - 1, step, 0)
        lax.fori_loop(0, cells - 2 - cell, lambda n, carry: step(cells - 1 - n, carry), 0)

    loads = [
        pltpu.make_async_copy(src, dst, load_sem.at[n])
        for n, (src, dst) in enumerate(zip(args, held))
    ]
    for n in (3, 5, 4, 8, 0, 1, 2, 6, 7, 9):
        loads[n].start()
    greet_near()

    def clear(slot):
        for buf, rows, _ in [site_msg, point_msg] + mu_msg + charge_msg[1:]:
            buf[slot * grps * rows : (slot + 1) * grps * rows] = jnp.zeros((grps * rows, 1, BLOCK), jnp.float32)

    for it in range(ITERS):
        for g in range(grps):
            for c in (lax.max(cell - 1, 0), cell, lax.min(cell + 1, cells - 1)):
                tab[it][g * cells + c] = jnp.zeros((1, BLOCK), jnp.float32)
    pl.when(jnp.logical_not(has_prev))(lambda: clear(0))
    pl.when(jnp.logical_not(has_next))(lambda: clear(2))

    greeted = [(has_prev, grps), (has_next, grps), (has_prev2, 1), (has_next2, 1)]
    pl.semaphore_wait(barrier, grps - 1 + sum(n * met.astype(jnp.int32) for met, n in greeted))
    edge_up, edge_down = jnp.logical_not(has_prev2), jnp.logical_not(has_next2)

    @pl.when(jnp.logical_and(edge_up, has_next2))
    def _():
        pl.semaphore_signal(upward, inc=1, device_id=(cell + 2, grp), device_id_type=MESH)

    @pl.when(jnp.logical_and(edge_down, has_prev2))
    def _():
        pl.semaphore_signal(downward, inc=1, device_id=(cell - 2, grp), device_id_type=MESH)

    for n in (3, 5, 4, 8):
        loads[n].wait()

    for b in range(na):
        for a in range(3):
            sit[own * 3 * na + b * 3 + a] = vec_row(sites, a, b)
            mus[0][own * 3 * na + b * 3 + a] = vec_row(guess, a, b)
    for b in range(ng):
        for a in range(3):
            pts[own * 4 * ng + b * 4 + a] = vec_row(points, a, b)
        pts[own * 4 * ng + b * 4 + 3] = flat_row(base, b)

    def inverse_of(dx, dy, dz):
        return lax.rsqrt(dx * dx + dy * dy + dz * dz + soften_sq)

    def store_dipole_pair(ref, slot, targets, source, self_mask):
        dx, dy, dz = (t - s for t, s in zip(targets, source))
        inv = inverse_of(dx, dy, dz)
        cube = inv * inv * inv
        weight = inv * math.sqrt(3.0)
        ref[slot] = dx * weight
        ref[slot + 1] = dy * weight
        ref[slot + 2] = dz * weight
        ref[slot + 3] = cube if self_mask is None else jnp.where(self_mask, 0.0, cube)

    def store_charge_pair(ref, slot, targets, source):
        dx, dy, dz = (t - s for t, s in zip(targets, source))
        inv = inverse_of(dx, dy, dz)
        cube = inv * inv * inv
        ref[slot] = dx * cube
        ref[slot + 1] = dy * cube
        ref[slot + 2] = dz * cube

    def column_sum(x):
        return jnp.sum(x, axis=0, keepdims=True)

    def wide(row):
        return jnp.broadcast_to(row, (SUB, BLOCK))

    def targets_of(ref, b, group):
        return [ref[b, a, pl.ds(group * SUB, SUB), :] for a in range(3)]

    def piece_copy(msg, slot, c, g):
        buf, rows, kind = msg
        return pltpu.make_async_remote_copy(
            src_ref=buf.at[pl.ds(own * rows, rows)],
            dst_ref=buf.at[pl.ds((slot * grps + grp) * rows, rows)],
            send_sem=send_sem.at[kind],
            recv_sem=recv_sem.at[kind],
            device_id=(c, g),
            device_id_type=MESH,
        )

    def for_all(msg, act):
        @pl.when(has_prev)
        def _():
            for d in order:
                g = lax.rem(grp + d, grps)
                act(piece_copy(msg, 2, cell - 1, g))

        @pl.when(has_next)
        def _():
            for d in order:
                g = lax.rem(grp + d, grps)
                act(piece_copy(msg, 0, cell + 1, g))

        for d in order:
            if d:
                g = lax.rem(grp + d, grps)
                act(piece_copy(msg, 1, cell, g))

    inner = jnp.logical_and(has_prev, has_next)

    def traffic(msg, act):
        buf, rows, kind = msg

        def part(n):
            some = buf.at[pl.ds(0, n * rows)]
            act(
                pltpu.make_async_remote_copy(
                    src_ref=some,
                    dst_ref=some,
                    send_sem=send_sem.at[kind],
                    recv_sem=recv_sem.at[kind],
                    device_id=(cell, lax.rem(grp + 1, grps)),
                    device_id_type=MESH,
                )
            )

        pl.when(inner)(lambda: part(3 * grps - 1))
        pl.when(jnp.logical_not(inner))(lambda: part(2 * grps - 1))

    def all_arrive(msg):
        traffic(msg, arrive)

    def start(copy):
        copy.start()

    def arrive(copy):
        copy.wait_recv()

    def finish(copy):
        copy.wait_send()

    def far_row(it, c, g):
        return tab[it].at[pl.ds(g * cells + c, 1)]

    def far_copy(it, c, g):
        return pltpu.make_async_remote_copy(
            src_ref=far_row(it, cell, grp),
            dst_ref=far_row(it, cell, grp),
            send_sem=far_send.at[it],
            recv_sem=far_recv.at[it],
            device_id=(c, g),
            device_id_type=MESH,
        )

    def far_all(it, act):
        pl.when(inner)(lambda: act(far_rows(it, cells - 3)))
        pl.when(jnp.logical_not(inner))(lambda: act(far_rows(it, cells - 2)))

    def far_rows(it, n):
        rows = tab[it].at[pl.ds(0, n * grps)]
        return pltpu.make_async_remote_copy(
            src_ref=rows,
            dst_ref=rows,
            send_sem=far_send.at[it],
            recv_sem=far_recv.at[it],
            device_id=(lax.rem(cell + 1, cells), grp),
            device_id_type=MESH,
        )

    def charge_row(it, w):
        return pts[w * 4 + 3] if it == 0 else chg[it][w]

    def own_sums(it):
        rows = []
        for a in range(3):
            total = mus[it][own * 3 * na + a]
            for b in range(1, na):
                total = total + mus[it][own * 3 * na + b * 3 + a]
            rows.append(total)
        q = [charge_row(it, own * ng + b) for b in range(ng)]
        rows.append(functools.reduce(jnp.add, q))
        for a in range(3):
            rows.append(functools.reduce(jnp.add, [q[b] * (vec_row(points, a, b) - centre[a]) for b in range(ng)]))
        tile = jnp.zeros((SUB, BLOCK), jnp.float32)
        for n, row in enumerate(rows):
            tile = jnp.where(subs == n, wide(row), tile)
        sums = jnp.sum(tile, axis=1, keepdims=True)
        tab[it][grp * cells + cell] = column_sum(jnp.where(diag == 0, sums, 0.0))

    def far_sums(it):
        parts = []
        for first in range(0, cells, SUB):
            part = jnp.zeros((SUB, BLOCK), jnp.float32)
            for c in range(first, min(first + SUB, cells)):
                row = functools.reduce(jnp.add, [wide(tab[it][g * cells + c]) for g in range(grps)])
                part = jnp.where(subs == c - first, row, part)
            parts.append(part)
        total = jnp.concatenate(parts, axis=0)[:cells]
        return [jnp.broadcast_to(total[:, n : n + 1], (cells, BLOCK)) for n in range(7)]

    def site_rows(w):
        return [wide(sit[w * 3 + a]) for a in range(3)]

    def point_rows(w):
        return [wide(pts[w * 4 + a]) for a in range(3)]

    def mu_rows(it, w):
        return [wide(mus[it][w * 3 + a]) for a in range(3)]

    def near_geometry(i, carry):
        b = lax.div(i, HALVES)
        first = lax.rem(i, HALVES) * UNROLL
        for k in range(nb):
            source = site_rows(near_s[b, k])
            for t in range(UNROLL):
                slot = ((i * UNROLL + t) * nb + k) * 4
                store_dipole_pair(geo, slot, targets_of(tgt_a, b, first + t), source, None)
        return carry

    def charge_geometry(i, carry):
        b = lax.div(i, HALVES)
        first = lax.rem(i, HALVES) * UNROLL
        for k in range(nq):
            source = point_rows(grid_s[b, k])
            for t in range(UNROLL):
                slot = ((i * UNROLL + t) * nq + k) * 3
                store_charge_pair(cgeo, slot, targets_of(tgt_a, b, first + t), source)
        return carry

    def grid_geometry(i, carry):
        b = lax.div(i, HALVES)
        first = lax.rem(i, HALVES) * UNROLL
        for k in range(nm):
            source = site_rows(source_s[b, k])
            for t in range(UNROLL):
                slot = ((i * UNROLL + t) * nm + k) * 3
                store_charge_pair(pgeo, slot, targets_of(tgt_g, b, first + t), source)
        return carry

    def self_atoms(it, i, carry):
        b = lax.div(i, HALVES)
        mu = mu_rows(it, own * na + b)
        for t in range(UNROLL):
            slot = (i * UNROLL + t) * 4
            u = [sgeo[slot + a] for a in range(3)]
            cube = sgeo[slot + 3]
            proj = u[0] * mu[0] + u[1] * mu[1] + u[2] * mu[2]
            for a in range(3):
                acc_a[(i * UNROLL + t) * 3 + a] = cube * (u[a] * proj - mu[a])
        return carry

    def near_atoms(it, i, carry):
        b = lax.div(i, HALVES)
        acc = [[acc_a[(i * UNROLL + t) * 3 + a] for a in range(3)] for t in range(UNROLL)]
        for k in range(nb):
            mu = mu_rows(it, near_s[b, k])
            for t in range(UNROLL):
                slot = ((i * UNROLL + t) * nb + k) * 4
                u = [geo[slot + a] for a in range(3)]
                cube = geo[slot + 3]
                proj = u[0] * mu[0] + u[1] * mu[1] + u[2] * mu[2]
                for a in range(3):
                    acc[t][a] = acc[t][a] + cube * (u[a] * proj - mu[a])
        for t in range(UNROLL):
            for a in range(3):
                acc_a[(i * UNROLL + t) * 3 + a] = acc[t][a]
        return carry

    def near_grid(it, i, carry):
        b = lax.div(i, HALVES)
        acc = [None] * UNROLL
        for k in range(nm):
            mu = mu_rows(it, source_s[b, k])
            for t in range(UNROLL):
                slot = ((i * UNROLL + t) * nm + k) * 3
                term = pgeo[slot] * mu[0] + pgeo[slot + 1] * mu[1] + pgeo[slot + 2] * mu[2]
                acc[t] = term if k == 0 else acc[t] + term
        for t in range(UNROLL):
            acc_g[i * UNROLL + t] = acc[t]
        return carry

    def gather_lanes(tiles):
        row = jnp.zeros((SUB, BLOCK), jnp.float32)
        for t, tile in enumerate(tiles):
            total = jnp.sum(tile, axis=1, keepdims=True)
            row = jnp.where(diag == t * SUB, total, row)
        return column_sum(row)

    def atom_fields(it):
        rows = []
        for b in range(na):
            q = [wide(charge_row(it, grid_s[b, k])) for k in range(nq)]
            tiles = [[], [], []]
            for t in range(GROUPS):
                n = b * GROUPS + t
                for a in range(3):
                    terms = [cgeo[(n * nq + k) * 3 + a] * q[k] for k in range(nq)]
                    tiles[a].append(acc_a[n * 3 + a] + functools.reduce(jnp.add, terms))
            rows.append([gather_lanes(tiles[a]) for a in range(3)])
        return rows

    def grid_fields():
        return [gather_lanes([acc_g[b * GROUPS + t] for t in range(GROUPS)]) for b in range(ng)]

    def store_far(ref, n, row_of):
        c = lax.broadcasted_iota(jnp.int32, (cells, BLOCK), 0)
        dx = row_of(0) - (c.astype(jnp.float32) + 0.5)
        dy = jnp.broadcast_to(row_of(1) - 0.5, (cells, BLOCK))
        dz = jnp.broadcast_to(row_of(2) - 0.5, (cells, BLOCK))
        inv = inverse_of(dx, dy, dz)
        cube = jnp.where(jnp.abs(c - cell) >= 2, inv * inv * inv, 0.0)
        for m, x in enumerate((dx, dy, dz, cube, cube * inv * inv * 3.0)):
            ref[n * 5 + m] = x

    def finish_atoms(it, near, sums):
        moments = [sums[a] + sums[4 + a] for a in range(3)]
        for b in range(na):
            delta = [fgeo_a[b * 5 + a] for a in range(3)]
            cube, fifth = fgeo_a[b * 5 + 3], fgeo_a[b * 5 + 4]
            radial = fifth * (moments[0] * delta[0] + moments[1] * delta[1] + moments[2] * delta[2])
            radial = radial + sums[3] * cube
            for a in range(3):
                far = column_sum(radial * delta[a] - moments[a] * cube)
                new = flat_row(pol, b) * (vec_row(fixed, a, b) + (near[b][a] + far))
                if it + 1 < ITERS:
                    mus[it + 1][own * 3 * na + b * 3 + a] = new
                else:
                    out_dip[a : a + 1, b * BLOCK : (b + 1) * BLOCK] = new

    def finish_grid(it, near, sums):
        for b in range(ng):
            delta = [fgeo_g[b * 5 + a] for a in range(3)]
            proj = sums[0] * delta[0] + sums[1] * delta[1] + sums[2] * delta[2]
            far = column_sum(proj * fgeo_g[b * 5 + 3])
            new = flat_row(base, b) - flat_row(resp, b) * (near[b] + far)
            if it + 1 < ITERS:
                chg[it + 1][own * ng + b] = new
            else:
                out_q[b * BLOCK : (b + 1) * BLOCK] = new.reshape(BLOCK)

    def repeat(n, chunk, fn):
        def step(j, carry):
            for m in range(chunk):
                fn(j * chunk + m, carry)
            return carry

        if chunk == n:
            step(0, 0)
        else:
            lax.fori_loop(0, n // chunk, step, 0)

    atom_steps, grid_steps = na * HALVES, ng * HALVES

    for_all(site_msg, start)
    for_all(mu_msg[0], start)
    for_all(point_msg, start)
    own_sums(0)

    @pl.when(has_prev2)
    def _():
        pl.semaphore_wait(upward, 1)

    @pl.when(jnp.logical_and(has_prev2, has_next2))
    def _():
        pl.semaphore_signal(upward, inc=1, device_id=(cell + 2, grp), device_id_type=MESH)

    @pl.when(has_next2)
    def _():
        pl.semaphore_wait(downward, 1)

    @pl.when(jnp.logical_and(has_prev2, has_next2))
    def _():
        pl.semaphore_signal(downward, inc=1, device_id=(cell - 2, grp), device_id_type=MESH)

    each_far_cell(lambda c, g: far_copy(0, c, g).start())

    for a in range(3):
        for b in range(na):
            tgt_a[b, a] = jnp.transpose(jnp.broadcast_to(vec_row(sites, a, b), (BLOCK, BLOCK)))
        for b in range(ng):
            tgt_g[b, a] = jnp.transpose(jnp.broadcast_to(vec_row(points, a, b), (BLOCK, BLOCK)))
    for b in range(na):
        source = [wide(vec_row(sites, a, b)) for a in range(3)]
        for t in range(GROUPS):
            store_dipole_pair(sgeo, (b * GROUPS + t) * 4, targets_of(tgt_a, b, t), source, diag == t * SUB)
    repeat(atom_steps, 4, functools.partial(self_atoms, 0))
    for b in range(na):
        store_far(fgeo_a, b, lambda a: vec_row(sites, a, b))
    for b in range(ng):
        store_far(fgeo_g, b, lambda a: vec_row(points, a, b))
    for n in (0, 1, 2, 6, 7, 9):
        loads[n].wait()

    all_arrive(site_msg)
    repeat(atom_steps, 4, near_geometry)

    for it in range(ITERS):
        last = it + 1 == ITERS
        all_arrive(mu_msg[it])
        repeat(atom_steps, 4, functools.partial(near_atoms, it))
        if it:
            repeat(grid_steps, 3, functools.partial(near_grid, it))
        if it == 0:
            all_arrive(point_msg)
            repeat(atom_steps, 4, charge_geometry)
        else:
            all_arrive(charge_msg[it])
        atom_near = atom_fields(it)
        grid_near = grid_fields() if it else None
        far_all(it, arrive)
        sums = far_sums(it)
        finish_atoms(it, atom_near, sums)
        if last:
            finish_grid(it, grid_near, sums)
            break
        for_all(mu_msg[it + 1], start)
        if it == 0:
            repeat(grid_steps, 3, grid_geometry)
            repeat(grid_steps, 3, functools.partial(near_grid, it))
            grid_near = grid_fields()
        finish_grid(it, grid_near, sums)
        own_sums(it + 1)
        each_far_cell(lambda c, g: far_copy(it + 1, c, g).start())
        for_all(charge_msg[it + 1], start)
        repeat(atom_steps, 4, functools.partial(self_atoms, it + 1))

    for msg in [site_msg, point_msg] + mu_msg + charge_msg[1:]:
        traffic(msg, finish)
    for it in range(ITERS):
        far_all(it, finish)


def hand_over(dip, q, out_dip, out_q, sem):
    copies = [
        pltpu.make_async_copy(dip, out_dip, sem.at[0]),
        pltpu.make_async_copy(q, out_q, sem.at[1]),
    ]
    for copy in copies:
        copy.start()
    for copy in copies:
        copy.wait()


def solution(mesh):
    cells, grps = mesh.shape["cell"], mesh.shape["grp"]

    def step(sites, points, guess, fixed, pol, base, resp, near, grid, source):
        na, nb = near.shape
        nq = grid.shape[1]
        ng, nm = source.shape
        f32 = jnp.float32
        args = (near, grid, source, sites, points, guess, fixed, pol, base, resp)
        args = tuple(pltpu.with_memory_space_constraint(x, pltpu.HBM) for x in args)
        vmem = pl.BlockSpec(memory_space=pltpu.VMEM)
        hbm = pl.BlockSpec(memory_space=pltpu.HBM)
        dma = pltpu.SemaphoreType.DMA
        outs = (jax.ShapeDtypeStruct(sites.shape, f32), jax.ShapeDtypeStruct(base.shape, f32))

        def rows(n):
            return pltpu.VMEM((3 * grps * n, 1, BLOCK), f32)

        def tiles(n, height=SUB):
            return pltpu.VMEM((n, height, BLOCK), f32)

        kinds = 1 + 2 * ITERS
        results = pl.pallas_call(
            functools.partial(body, (cells, grps, na, ng, nb, nq, nm)),
            out_shape=outs,
            in_specs=[hbm] * 10,
            out_specs=(vmem, vmem),
            scratch_shapes=[pltpu.SMEM(x.shape, x.dtype) for x in args[:3]]
            + [pltpu.VMEM(x.shape, x.dtype) for x in args[3:]]
            + [rows(3 * na), rows(4 * ng)]
            + [rows(3 * na) for _ in range(ITERS)]
            + [rows(ng) for _ in range(ITERS - 1)]
            + [pltpu.VMEM((cells * grps, 1, BLOCK), f32) for _ in range(ITERS)]
            + [
                pltpu.VMEM((na, 3, BLOCK, BLOCK), f32),
                pltpu.VMEM((ng, 3, BLOCK, BLOCK), f32),
                tiles(na * GROUPS * nb * 4),
                tiles(na * GROUPS * 4),
                tiles(na * GROUPS * nq * 3),
                tiles(ng * GROUPS * nm * 3),
                tiles(na * 5, cells),
                tiles(ng * 5, cells),
                tiles(na * GROUPS * 3),
                tiles(ng * GROUPS),
                dma((10,)),
                dma((kinds,)),
                dma((kinds,)),
                dma((ITERS,)),
                dma((ITERS,)),
                pltpu.SemaphoreType.REGULAR,
                pltpu.SemaphoreType.REGULAR,
            ],
            compiler_params=pltpu.CompilerParams(
                collective_id=0, has_side_effects=True, vmem_limit_bytes=40 << 20
            ),
        )(*args)
        return pl.pallas_call(
            hand_over,
            out_shape=outs,
            in_specs=[vmem, vmem],
            out_specs=(hbm, hbm),
            scratch_shapes=[dma((2,))],
            compiler_params=pltpu.CompilerParams(vmem_limit_bytes=1 << 20),
        )(*results)

    pair = P(("cell", "grp"))
    wide = P(None, ("cell", "grp"))
    tall = P(("cell", "grp"), None)
    return jax.shard_map(
        step,
        mesh=mesh,
        in_specs=(wide, wide, wide, wide, pair, pair, pair, tall, tall, tall),
        out_specs=(wide, pair),
        check_vma=False,
    )
```

```python
import functools
import math

import jax
import jax.numpy as jnp
from jax import lax
from jax.experimental import pallas as pl
from jax.experimental.pallas import tpu as pltpu
from jax.sharding import PartitionSpec as P

BLOCK = 128
SUB = 8
GROUPS = BLOCK // SUB
UNROLL = 8
HALVES = GROUPS // UNROLL
ITERS = 3
MESH = pl.DeviceIdType.MESH

soften_sq = 0.04


def body(dims, *refs):
    cells, grps, na, ng, nb, nq, nm = dims
    args, (out_dip, out_q), held = refs[:10], refs[10:12], refs[12:22]
    near_s, grid_s, source_s, sites, points, guess, fixed, pol, base, resp = held
    sit, pts = refs[22:24]
    mus = refs[24 : 24 + ITERS]
    chg = (None,) + refs[24 + ITERS : 23 + 2 * ITERS]
    tab = refs[23 + 2 * ITERS : 23 + 3 * ITERS]
    rest = refs[23 + 3 * ITERS :]
    tgt_a, tgt_g, geo, sgeo, cgeo, pgeo, fgeo_a, fgeo_g, acc_a, acc_g, kept = rest[:11]
    load_sem, send_sem, recv_sem, far_send, far_recv, upward, downward = rest[11:]
    cell = lax.axis_index("cell")
    grp = lax.axis_index("grp")
    has_prev = cell > 0
    has_next = cell < cells - 1
    has_prev2 = cell > 1
    has_next2 = cell < cells - 2
    own = grps + grp
    cell_f = cell.astype(jnp.float32)
    centre = (cell_f + 0.5, 0.5, 0.5)
    pieces = 3 * grps
    order = sorted(range(grps), key=lambda d: (abs(2 * d - grps), d))

    site_msg = (sit, 3 * na, 0)
    point_msg = (pts, 4 * ng, 1)
    mu_msg = [(mus[it], 3 * na, 2 + it) for it in range(ITERS)]
    charge_msg = [None] + [(chg[it], ng, 1 + ITERS + it) for it in range(1, ITERS)]

    def vec_row(ref, a, b):
        return ref[a : a + 1, b * BLOCK : (b + 1) * BLOCK]

    def flat_row(ref, b):
        return ref[b * BLOCK : (b + 1) * BLOCK].reshape(1, BLOCK)

    lanes = lax.broadcasted_iota(jnp.int32, (SUB, BLOCK), 1)
    subs = lax.broadcasted_iota(jnp.int32, (SUB, BLOCK), 0)
    diag = lanes - subs

    barrier = pltpu.get_barrier_semaphore()

    def greet(c, g):
        pl.semaphore_signal(barrier, inc=1, device_id=(c, g), device_id_type=MESH)

    def greet_near():
        @pl.when(has_prev2)
        def _():
            greet(cell - 2, grp)

        @pl.when(has_prev)
        def _():
            for d in order:
                greet(cell - 1, lax.rem(grp + d, grps))

        @pl.when(has_next)
        def _():
            for d in order:
                greet(cell + 1, lax.rem(grp + d, grps))

        for d in range(1, grps):
            greet(cell, lax.rem(grp + d, grps))

        @pl.when(has_next2)
        def _():
            greet(cell + 2, grp)

    def each_far_cell(act):
        def step(c, carry):
            for d in order:
                act(c, lax.rem(grp + d, grps))
            return carry

        lax.fori_loop(0, cell - 1, step, 0)
        lax.fori_loop(0, cells - 2 - cell, lambda n, carry: step(cells - 1 - n, carry), 0)

    loads = [
        pltpu.make_async_copy(src, dst, load_sem.at[n])
        for n, (src, dst) in enumerate(zip(args, held))
    ]
    for n in (3, 5, 4, 8, 0, 1, 2, 6, 7, 9):
        loads[n].start()
    greet_near()

    def clear(slot):
        for buf, rows, _ in [site_msg, point_msg] + mu_msg + charge_msg[1:]:
            buf[slot * grps * rows : (slot + 1) * grps * rows] = jnp.zeros((grps * rows, 1, BLOCK), jnp.float32)

    for it in range(ITERS):
        for g in range(grps):
            for c in (lax.max(cell - 1, 0), cell, lax.min(cell + 1, cells - 1)):
                tab[it][g * cells + c] = jnp.zeros((1, BLOCK), jnp.float32)
    pl.when(jnp.logical_not(has_prev))(lambda: clear(0))
    pl.when(jnp.logical_not(has_next))(lambda: clear(2))

    greeted = [(has_prev, grps), (has_next, grps), (has_prev2, 1), (has_next2, 1)]
    pl.semaphore_wait(barrier, grps - 1 + sum(n * met.astype(jnp.int32) for met, n in greeted))
    edge_up, edge_down = jnp.logical_not(has_prev2), jnp.logical_not(has_next2)

    @pl.when(jnp.logical_and(edge_up, has_next2))
    def _():
        pl.semaphore_signal(upward, inc=1, device_id=(cell + 2, grp), device_id_type=MESH)

    @pl.when(jnp.logical_and(edge_down, has_prev2))
    def _():
        pl.semaphore_signal(downward, inc=1, device_id=(cell - 2, grp), device_id_type=MESH)

    for n in (3, 5, 4, 8):
        loads[n].wait()

    for b in range(na):
        for a in range(3):
            sit[own * 3 * na + b * 3 + a] = vec_row(sites, a, b)
            mus[0][own * 3 * na + b * 3 + a] = vec_row(guess, a, b)
    for b in range(ng):
        for a in range(3):
            pts[own * 4 * ng + b * 4 + a] = vec_row(points, a, b)
        pts[own * 4 * ng + b * 4 + 3] = flat_row(base, b)

    def inverse_of(dx, dy, dz):
        return lax.rsqrt(dx * dx + dy * dy + dz * dz + soften_sq)

    def store_dipole_pair(ref, slot, targets, source, self_mask):
        dx, dy, dz = (t - s for t, s in zip(targets, source))
        inv = inverse_of(dx, dy, dz)
        cube = inv * inv * inv
        weight = inv * math.sqrt(3.0)
        ref[slot] = dx * weight
        ref[slot + 1] = dy * weight
        ref[slot + 2] = dz * weight
        ref[slot + 3] = cube if self_mask is None else jnp.where(self_mask, 0.0, cube)

    def store_charge_pair(ref, slot, targets, source):
        dx, dy, dz = (t - s for t, s in zip(targets, source))
        inv = inverse_of(dx, dy, dz)
        cube = inv * inv * inv
        ref[slot] = dx * cube
        ref[slot + 1] = dy * cube
        ref[slot + 2] = dz * cube

    def column_sum(x):
        return jnp.sum(x, axis=0, keepdims=True)

    def wide(row):
        return jnp.broadcast_to(row, (SUB, BLOCK))

    def targets_of(ref, b, group):
        return [ref[b, a, pl.ds(group * SUB, SUB), :] for a in range(3)]

    def piece_copy(msg, slot, c, g):
        buf, rows, kind = msg
        return pltpu.make_async_remote_copy(
            src_ref=buf.at[pl.ds(own * rows, rows)],
            dst_ref=buf.at[pl.ds((slot * grps + grp) * rows, rows)],
            send_sem=send_sem.at[kind],
            recv_sem=recv_sem.at[kind],
            device_id=(c, g),
            device_id_type=MESH,
        )

    def for_all(msg, act):
        @pl.when(has_prev)
        def _():
            for d in order:
                g = lax.rem(grp + d, grps)
                act(piece_copy(msg, 2, cell - 1, g))

        @pl.when(has_next)
        def _():
            for d in order:
                g = lax.rem(grp + d, grps)
                act(piece_copy(msg, 0, cell + 1, g))

        for d in order:
            if d:
                g = lax.rem(grp + d, grps)
                act(piece_copy(msg, 1, cell, g))

    inner = jnp.logical_and(has_prev, has_next)

    def traffic(msg, act):
        buf, rows, kind = msg

        def part(n):
            some = buf.at[pl.ds(0, n * rows)]
            act(
                pltpu.make_async_remote_copy(
                    src_ref=some,
                    dst_ref=some,
                    send_sem=send_sem.at[kind],
                    recv_sem=recv_sem.at[kind],
                    device_id=(cell, lax.rem(grp + 1, grps)),
                    device_id_type=MESH,
                )
            )

        pl.when(inner)(lambda: part(3 * grps - 1))
        pl.when(jnp.logical_not(inner))(lambda: part(2 * grps - 1))

    def all_arrive(msg):
        traffic(msg, arrive)

    def start(copy):
        copy.start()

    def arrive(copy):
        copy.wait_recv()

    def finish(copy):
        copy.wait_send()

    def far_row(it, c, g):
        return tab[it].at[pl.ds(g * cells + c, 1)]

    def far_copy(it, c, g):
        return pltpu.make_async_remote_copy(
            src_ref=far_row(it, cell, grp),
            dst_ref=far_row(it, cell, grp),
            send_sem=far_send.at[it],
            recv_sem=far_recv.at[it],
            device_id=(c, g),
            device_id_type=MESH,
        )

    def far_all(it, act):
        pl.when(inner)(lambda: act(far_rows(it, cells - 3)))
        pl.when(jnp.logical_not(inner))(lambda: act(far_rows(it, cells - 2)))

    def far_rows(it, n):
        rows = tab[it].at[pl.ds(0, n * grps)]
        return pltpu.make_async_remote_copy(
            src_ref=rows,
            dst_ref=rows,
            send_sem=far_send.at[it],
            recv_sem=far_recv.at[it],
            device_id=(lax.rem(cell + 1, cells), grp),
            device_id_type=MESH,
        )

    def charge_row(it, w):
        return pts[w * 4 + 3] if it == 0 else chg[it][w]

    def own_sums(it):
        rows = []
        for a in range(3):
            total = mus[it][own * 3 * na + a]
            for b in range(1, na):
                total = total + mus[it][own * 3 * na + b * 3 + a]
            rows.append(total)
        q = [charge_row(it, own * ng + b) for b in range(ng)]
        rows.append(functools.reduce(jnp.add, q))
        for a in range(3):
            rows.append(functools.reduce(jnp.add, [q[b] * (vec_row(points, a, b) - centre[a]) for b in range(ng)]))
        tile = jnp.zeros((SUB, BLOCK), jnp.float32)
        for n, row in enumerate(rows):
            tile = jnp.where(subs == n, wide(row), tile)
        sums = jnp.sum(tile, axis=1, keepdims=True)
        tab[it][grp * cells + cell] = column_sum(jnp.where(diag == 0, sums, 0.0))

    def far_sums(it):
        parts = []
        for first in range(0, cells, SUB):
            part = jnp.zeros((SUB, BLOCK), jnp.float32)
            for c in range(first, min(first + SUB, cells)):
                row = functools.reduce(jnp.add, [wide(tab[it][g * cells + c]) for g in range(grps)])
                part = jnp.where(subs == c - first, row, part)
            parts.append(part)
        total = jnp.concatenate(parts, axis=0)[:cells]
        return [jnp.broadcast_to(total[:, n : n + 1], (cells, BLOCK)) for n in range(7)]

    def site_rows(w):
        return [wide(sit[w * 3 + a]) for a in range(3)]

    def point_rows(w):
        return [wide(pts[w * 4 + a]) for a in range(3)]

    def mu_rows(it, w):
        return [wide(mus[it][w * 3 + a]) for a in range(3)]

    def near_geometry(i, carry):
        b = lax.div(i, HALVES)
        first = lax.rem(i, HALVES) * UNROLL
        for k in range(nb):
            source = site_rows(near_s[b, k])
            for t in range(UNROLL):
                slot = ((i * UNROLL + t) * nb + k) * 4
                store_dipole_pair(geo, slot, targets_of(tgt_a, b, first + t), source, None)
        return carry

    def charge_geometry(i, carry):
        b = lax.div(i, HALVES)
        first = lax.rem(i, HALVES) * UNROLL
        for k in range(nq):
            source = point_rows(grid_s[b, k])
            for t in range(UNROLL):
                slot = ((i * UNROLL + t) * nq + k) * 3
                store_charge_pair(cgeo, slot, targets_of(tgt_a, b, first + t), source)
        return carry

    def grid_geometry(i, carry):
        b = lax.div(i, HALVES)
        first = lax.rem(i, HALVES) * UNROLL
        for k in range(nm):
            source = site_rows(source_s[b, k])
            for t in range(UNROLL):
                slot = ((i * UNROLL + t) * nm + k) * 3
                store_charge_pair(pgeo, slot, targets_of(tgt_g, b, first + t), source)
        return carry

    def self_atoms(it, i, carry):
        b = lax.div(i, HALVES)
        mu = mu_rows(it, own * na + b)
        for t in range(UNROLL):
            slot = (i * UNROLL + t) * 4
            u = [sgeo[slot + a] for a in range(3)]
            cube = sgeo[slot + 3]
            proj = u[0] * mu[0] + u[1] * mu[1] + u[2] * mu[2]
            for a in range(3):
                acc_a[(i * UNROLL + t) * 3 + a] = cube * (u[a] * proj - mu[a])
        return carry

    def near_atoms(it, i, carry):
        b = lax.div(i, HALVES)
        acc = [[acc_a[(i * UNROLL + t) * 3 + a] for a in range(3)] for t in range(UNROLL)]
        for k in range(nb):
            mu = mu_rows(it, near_s[b, k])
            for t in range(UNROLL):
                slot = ((i * UNROLL + t) * nb + k) * 4
                u = [geo[slot + a] for a in range(3)]
                cube = geo[slot + 3]
                proj = u[0] * mu[0] + u[1] * mu[1] + u[2] * mu[2]
                for a in range(3):
                    acc[t][a] = acc[t][a] + cube * (u[a] * proj - mu[a])
        for t in range(UNROLL):
            for a in range(3):
                acc_a[(i * UNROLL + t) * 3 + a] = acc[t][a]
        return carry

    def near_grid(it, i, carry):
        b = lax.div(i, HALVES)
        acc = [None] * UNROLL
        for k in range(nm):
            mu = mu_rows(it, source_s[b, k])
            for t in range(UNROLL):
                slot = ((i * UNROLL + t) * nm + k) * 3
                term = pgeo[slot] * mu[0] + pgeo[slot + 1] * mu[1] + pgeo[slot + 2] * mu[2]
                acc[t] = term if k == 0 else acc[t] + term
        for t in range(UNROLL):
            acc_g[i * UNROLL + t] = acc[t]
        return carry

    def gather_lanes(tiles):
        row = jnp.zeros((SUB, BLOCK), jnp.float32)
        for t, tile in enumerate(tiles):
            total = jnp.sum(tile, axis=1, keepdims=True)
            row = jnp.where(diag == t * SUB, total, row)
        return column_sum(row)

    def atom_fields(it):
        rows = []
        for b in range(na):
            q = [wide(charge_row(it, grid_s[b, k])) for k in range(nq)]
            tiles = [[], [], []]
            for t in range(GROUPS):
                n = b * GROUPS + t
                for a in range(3):
                    terms = [cgeo[(n * nq + k) * 3 + a] * q[k] for k in range(nq)]
                    tiles[a].append(acc_a[n * 3 + a] + functools.reduce(jnp.add, terms))
            rows.append([gather_lanes(tiles[a]) for a in range(3)])
        return rows

    def grid_fields():
        return [gather_lanes([acc_g[b * GROUPS + t] for t in range(GROUPS)]) for b in range(ng)]

    def store_far(ref, n, row_of):
        c = lax.broadcasted_iota(jnp.int32, (cells, BLOCK), 0)
        dx = row_of(0) - (c.astype(jnp.float32) + 0.5)
        dy = jnp.broadcast_to(row_of(1) - 0.5, (cells, BLOCK))
        dz = jnp.broadcast_to(row_of(2) - 0.5, (cells, BLOCK))
        inv = inverse_of(dx, dy, dz)
        cube = jnp.where(jnp.abs(c - cell) >= 2, inv * inv * inv, 0.0)
        for m, x in enumerate((dx, dy, dz, cube, cube * inv * inv * 3.0)):
            ref[n * 5 + m] = x

    def finish_atoms(it, near, sums):
        moments = [sums[a] + sums[4 + a] for a in range(3)]
        for b in range(na):
            delta = [fgeo_a[b * 5 + a] for a in range(3)]
            cube, fifth = fgeo_a[b * 5 + 3], fgeo_a[b * 5 + 4]
            radial = fifth * (moments[0] * delta[0] + moments[1] * delta[1] + moments[2] * delta[2])
            radial = radial + sums[3] * cube
            for a in range(3):
                far = column_sum(radial * delta[a] - moments[a] * cube)
                new = kept[b * 3 + a] + flat_row(pol, b) * far
                if it + 1 < ITERS:
                    mus[it + 1][own * 3 * na + b * 3 + a] = new
                else:
                    out_dip[a : a + 1, b * BLOCK : (b + 1) * BLOCK] = new

    def finish_grid(it, near, sums):
        for b in range(ng):
            delta = [fgeo_g[b * 5 + a] for a in range(3)]
            proj = sums[0] * delta[0] + sums[1] * delta[1] + sums[2] * delta[2]
            far = column_sum(proj * fgeo_g[b * 5 + 3])
            if it:
                new = kept[na * 3 + b] - flat_row(resp, b) * far
            else:
                new = flat_row(base, b) - flat_row(resp, b) * (near[b] + far)
            if it + 1 < ITERS:
                chg[it + 1][own * ng + b] = new
            else:
                out_q[b * BLOCK : (b + 1) * BLOCK] = new.reshape(BLOCK)

    def repeat(n, chunk, fn):
        def step(j, carry):
            for m in range(chunk):
                fn(j * chunk + m, carry)
            return carry

        if chunk == n:
            step(0, 0)
        else:
            lax.fori_loop(0, n // chunk, step, 0)

    atom_steps, grid_steps = na * HALVES, ng * HALVES

    for_all(site_msg, start)
    for_all(mu_msg[0], start)
    for_all(point_msg, start)
    own_sums(0)

    @pl.when(has_prev2)
    def _():
        pl.semaphore_wait(upward, 1)

    @pl.when(jnp.logical_and(has_prev2, has_next2))
    def _():
        pl.semaphore_signal(upward, inc=1, device_id=(cell + 2, grp), device_id_type=MESH)

    @pl.when(has_next2)
    def _():
        pl.semaphore_wait(downward, 1)

    @pl.when(jnp.logical_and(has_prev2, has_next2))
    def _():
        pl.semaphore_signal(downward, inc=1, device_id=(cell - 2, grp), device_id_type=MESH)

    each_far_cell(lambda c, g: far_copy(0, c, g).start())

    for a in range(3):
        for b in range(na):
            tgt_a[b, a] = jnp.transpose(jnp.broadcast_to(vec_row(sites, a, b), (BLOCK, BLOCK)))
        for b in range(ng):
            tgt_g[b, a] = jnp.transpose(jnp.broadcast_to(vec_row(points, a, b), (BLOCK, BLOCK)))
    for b in range(na):
        source = [wide(vec_row(sites, a, b)) for a in range(3)]
        for t in range(GROUPS):
            store_dipole_pair(sgeo, (b * GROUPS + t) * 4, targets_of(tgt_a, b, t), source, diag == t * SUB)
    repeat(atom_steps, 4, functools.partial(self_atoms, 0))
    for b in range(na):
        store_far(fgeo_a, b, lambda a: vec_row(sites, a, b))
    for b in range(ng):
        store_far(fgeo_g, b, lambda a: vec_row(points, a, b))
    for n in (0, 1, 2, 6, 7, 9):
        loads[n].wait()

    all_arrive(site_msg)
    repeat(atom_steps, 4, near_geometry)

    for it in range(ITERS):
        last = it + 1 == ITERS
        all_arrive(mu_msg[it])
        repeat(atom_steps, 4, functools.partial(near_atoms, it))
        if it:
            repeat(grid_steps, 3, functools.partial(near_grid, it))
        if it == 0:
            all_arrive(point_msg)
            repeat(atom_steps, 4, charge_geometry)
        else:
            all_arrive(charge_msg[it])
        atom_near = atom_fields(it)
        grid_near = grid_fields() if it else None
        for b in range(na):
            for a in range(3):
                kept[b * 3 + a] = flat_row(pol, b) * (vec_row(fixed, a, b) + atom_near[b][a])
        if it:
            for b in range(ng):
                kept[na * 3 + b] = flat_row(base, b) - flat_row(resp, b) * grid_near[b]
        far_all(it, arrive)
        sums = far_sums(it)
        finish_atoms(it, atom_near, sums)
        if last:
            finish_grid(it, grid_near, sums)
            break
        for_all(mu_msg[it + 1], start)
        if it == 0:
            repeat(grid_steps, 3, grid_geometry)
            repeat(grid_steps, 3, functools.partial(near_grid, it))
            grid_near = grid_fields()
        finish_grid(it, grid_near, sums)
        own_sums(it + 1)
        each_far_cell(lambda c, g: far_copy(it + 1, c, g).start())
        for_all(charge_msg[it + 1], start)
        repeat(atom_steps, 4, functools.partial(self_atoms, it + 1))

    for msg in [site_msg, point_msg] + mu_msg + charge_msg[1:]:
        traffic(msg, finish)
    for it in range(ITERS):
        far_all(it, finish)


def hand_over(dip, q, out_dip, out_q, sem):
    copies = [
        pltpu.make_async_copy(dip, out_dip, sem.at[0]),
        pltpu.make_async_copy(q, out_q, sem.at[1]),
    ]
    for copy in copies:
        copy.start()
    for copy in copies:
        copy.wait()


def solution(mesh):
    cells, grps = mesh.shape["cell"], mesh.shape["grp"]

    def step(sites, points, guess, fixed, pol, base, resp, near, grid, source):
        na, nb = near.shape
        nq = grid.shape[1]
        ng, nm = source.shape
        f32 = jnp.float32
        args = (near, grid, source, sites, points, guess, fixed, pol, base, resp)
        args = tuple(pltpu.with_memory_space_constraint(x, pltpu.HBM) for x in args)
        vmem = pl.BlockSpec(memory_space=pltpu.VMEM)
        hbm = pl.BlockSpec(memory_space=pltpu.HBM)
        dma = pltpu.SemaphoreType.DMA
        outs = (jax.ShapeDtypeStruct(sites.shape, f32), jax.ShapeDtypeStruct(base.shape, f32))

        def rows(n):
            return pltpu.VMEM((3 * grps * n, 1, BLOCK), f32)

        def tiles(n, height=SUB):
            return pltpu.VMEM((n, height, BLOCK), f32)

        kinds = 1 + 2 * ITERS
        results = pl.pallas_call(
            functools.partial(body, (cells, grps, na, ng, nb, nq, nm)),
            out_shape=outs,
            in_specs=[hbm] * 10,
            out_specs=(vmem, vmem),
            scratch_shapes=[pltpu.SMEM(x.shape, x.dtype) for x in args[:3]]
            + [pltpu.VMEM(x.shape, x.dtype) for x in args[3:]]
            + [rows(3 * na), rows(4 * ng)]
            + [rows(3 * na) for _ in range(ITERS)]
            + [rows(ng) for _ in range(ITERS - 1)]
            + [pltpu.VMEM((cells * grps, 1, BLOCK), f32) for _ in range(ITERS)]
            + [
                pltpu.VMEM((na, 3, BLOCK, BLOCK), f32),
                pltpu.VMEM((ng, 3, BLOCK, BLOCK), f32),
                tiles(na * GROUPS * nb * 4),
                tiles(na * GROUPS * 4),
                tiles(na * GROUPS * nq * 3),
                tiles(ng * GROUPS * nm * 3),
                tiles(na * 5, cells),
                tiles(ng * 5, cells),
                tiles(na * GROUPS * 3),
                tiles(ng * GROUPS),
                pltpu.VMEM((na * 3 + ng, 1, BLOCK), f32),
                dma((10,)),
                dma((kinds,)),
                dma((kinds,)),
                dma((ITERS,)),
                dma((ITERS,)),
                pltpu.SemaphoreType.REGULAR,
                pltpu.SemaphoreType.REGULAR,
            ],
            compiler_params=pltpu.CompilerParams(
                collective_id=0, has_side_effects=True, vmem_limit_bytes=40 << 20
            ),
        )(*args)
        return pl.pallas_call(
            hand_over,
            out_shape=outs,
            in_specs=[vmem, vmem],
            out_specs=(hbm, hbm),
            scratch_shapes=[dma((2,))],
            compiler_params=pltpu.CompilerParams(vmem_limit_bytes=1 << 20),
        )(*results)

    pair = P(("cell", "grp"))
    wide = P(None, ("cell", "grp"))
    tall = P(("cell", "grp"), None)
    return jax.shard_map(
        step,
        mesh=mesh,
        in_specs=(wide, wide, wide, wide, pair, pair, pair, tall, tall, tall),
        out_specs=(wide, pair),
        check_vma=False,
    )
```
